32 devices in a mesh: il: 2 (over core), xl: 4 (over y, x), ta: 4 (over z).
Axes of the slice: x: 2, y: 2, z: 4, core: 2. Of those that a mesh axis runs over, the one named last changes fastest.
Arguments:
- traces: float32 [32, 832, 1024], P('il', 'xl', 'ta'), may hold values from -6 to 6
- bin_steps: int32 [2, 32, 832], P(None, 'il', 'xl'), may hold values from -1 to 1
Outputs:
- regridded: float32 [16, 416, 1536], P('il', 'xl', 'ta')
The draws below stay inside these ranges and needn't reach their ends.
Inputs may be any that keep to these rules, and one draw needn't show every extreme that they name: `bin_steps`: every entry is -1, 0 or 1.
All inputs are finite; a program needn't handle non-finite values.
Results may differ from the reference program's by a relative error of at most 0.0001.
Values sent between devices are 32-bit elements; how exact they have to be, the bound alone decides.
No kernel may reach another device: no remote copies, remote signals or barrier semaphores. Data moves between devices by JAX's collectives and lax.ppermute only.
A program may use at most 128 MiB of HBM per device.

```python
import jax
import jax.numpy as jnp
from jax import lax

CT = 256
TAPS = 16
P_SIZE = 3
Q = 2
NI = 32
NX = 832
NT = 1024
BI = 16
BX = 416
N_TA = 4


def set_ends(entries, own_key, low, largest):
    longest = entries.shape.index(max(entries.shape))
    spots = []
    for shift in (0, 1):
        where = [jax.random.randint(jax.random.fold_in(own_key, axis), (), 0, length) for axis, length in enumerate(entries.shape)]
        where[longest] = (where[longest] + shift) % entries.shape[longest]
        spots.append(tuple(where))
    return entries.at[spots[0]].set(low).at[spots[1]].set(largest)


def block_scale(key, shape, cuts, smallest, high):
    loudness, own = 1.0, jax.random.fold_in(key, 6)
    for dim, blocks in cuts:
        draws = jnp.exp(jax.random.uniform(jax.random.fold_in(own, dim), (blocks,), jnp.float32, smallest / len(cuts), high / len(cuts)))
        loudness = loudness * jnp.repeat(draws, shape[dim] // blocks).reshape([-1 if axis == dim else 1 for axis in range(len(shape))])
    return loudness


def gaussian(key, dims, spread, most, split=(), kind=jnp.bfloat16):
    drawn = spread * jax.random.normal(key, dims, jnp.float32)
    if split:
        drawn = drawn * block_scale(key, dims, split, -0.22, 0.18)
    return jnp.clip(drawn, -most, most).astype(kind)


def setup_inputs(seed: int = 0) -> dict:
    streams_of = jax.random.split(jax.random.key(seed), 3)
    traces = gaussian(streams_of[0], (NI, NX, NT), 1.0, 6.0, ((0, 2), (1, 4), (2, 4)), jnp.float32)
    bin_steps = set_ends(jax.random.randint(streams_of[1], (2, NI, NX), -1, 2), jax.random.fold_in(streams_of[1], 1), -1, 1).astype(jnp.int32)
    return {"traces": traces, "bin_steps": bin_steps}


def lanczos_table(row_count, col_count, tap_reach, ratio_p, ratio_q):
    row_ids = lax.broadcasted_iota(jnp.int32, (row_count, col_count), 0)
    col_ids = lax.broadcasted_iota(jnp.int32, (row_count, col_count), 1)
    offset = (col_ids * ratio_q - (row_ids - tap_reach) * ratio_p).astype(jnp.float32) / jnp.float32(ratio_p)
    inside = jnp.abs(offset) < jnp.float32(tap_reach)
    weights = jnp.sinc(offset) * jnp.sinc(offset / jnp.float32(tap_reach))
    return jnp.where(inside, weights, jnp.zeros_like(weights))


def reference(traces, bin_steps):
    tap_reach = TAPS // 2
    bin_total = jnp.zeros((BI + 2, BX + 2, NT), jnp.float32)
    fold_count = jnp.zeros((BI + 2, BX + 2), jnp.float32)
    for row_phase in (0, 1):
        for col_phase in (0, 1):
            sub_traces = traces[row_phase::2, col_phase::2]
            step_il = bin_steps[0, row_phase::2, col_phase::2]
            step_xl = bin_steps[1, row_phase::2, col_phase::2]
            for shift_il in (-1, 0, 1):
                for shift_xl in (-1, 0, 1):
                    chosen = ((step_il == shift_il) & (step_xl == shift_xl)).astype(jnp.float32)
                    widths = ((1 + shift_il, 1 - shift_il), (1 + shift_xl, 1 - shift_xl))
                    bin_total = bin_total + jnp.pad(sub_traces * chosen[:, :, None], widths + ((0, 0),))
                    fold_count = fold_count + jnp.pad(chosen, widths)
    stacked = bin_total[1:-1, 1:-1] / jnp.maximum(fold_count[1:-1, 1:-1], 1.0)[:, :, None]
    padded = jnp.pad(stacked, ((0, 0), (0, 0), (tap_reach, tap_reach)))
    taps_table = lanczos_table(CT + 2 * tap_reach, CT * P_SIZE // Q, tap_reach, P_SIZE, Q)
    blocks = []
    for block_idx in range(N_TA):
        block_rows = padded[:, :, block_idx * CT: block_idx * CT + CT + 2 * tap_reach].reshape(BI * BX, CT + 2 * tap_reach)
        result = jnp.dot(block_rows, taps_table, precision=lax.Precision.HIGHEST, preferred_element_type=jnp.float32)
        blocks.append(result.reshape(BI, BX, CT * P_SIZE // Q))
    return jnp.concatenate(blocks, axis=2)
```

```python
import functools

import jax
import jax.numpy as jnp
import numpy as np
from jax import lax
from jax.experimental import pallas as pl
from jax.experimental.pallas import tpu as pltpu
from jax.sharding import PartitionSpec as P

TAPS = 16
P_SIZE = 3
Q = 2
REACH = TAPS // 2
LANES = 128
F32 = jnp.float32
BF16 = jnp.bfloat16


def weight(x):
    inside = np.abs(x) < REACH
    return np.where(inside, np.sinc(x) * np.sinc(x / REACH), 0.0)


def split_table(table):
    high = table.astype(BF16)
    return high, (table - high.astype(np.float64)).astype(BF16)


def main_table(length):
    n = np.arange(length)[:, None]
    m = np.arange(length * P_SIZE // Q)[None, :]
    return weight((m * Q - n * P_SIZE) / P_SIZE)


def edge_table(length):
    out_len = length * P_SIZE // Q
    table = np.zeros((LANES, 2 * LANES))
    k = np.arange(REACH)[:, None]
    m = np.arange(LANES)[None, :]
    table[:REACH, :LANES] = weight((m * Q - (k - REACH) * P_SIZE) / P_SIZE)
    m = m + out_len - LANES
    table[LANES // 2 : LANES // 2 + REACH, LANES:] = weight((m * Q - (length + k) * P_SIZE) / P_SIZE)
    return table


def split(values):
    high = values.astype(BF16)
    return high, (values - high.astype(F32)).astype(BF16)


def dot(a, b, precision=None):
    return jnp.dot(a, b, precision=precision, preferred_element_type=F32)


def rim_kernel(traces, steps, left_out, right_out, left, right, sems):
    rows, cols, length = traces.shape
    copy_l = pltpu.make_async_copy(traces.at[:, 0:8, :], left, sems.at[0])
    copy_r = pltpu.make_async_copy(traces.at[:, cols - 8 : cols, :], right, sems.at[1])
    copy_l.start()
    copy_r.start()
    step_il = steps[0]
    step_xl = steps[1]
    masks = {}
    for side, spots in ((-1, (0, 1)), (1, (cols - 2, cols - 1))):
        for j in spots:
            for shift in (-1, 0, 1):
                hit = (step_xl[:, j : j + 1] == side) & (step_il[:, j : j + 1] == shift)
                masks[side, j, shift] = hit.astype(F32)
    copy_l.wait()
    copy_r.wait()
    parts = []
    for shift in (-1, 0, 1):
        row = []
        for side, buf, spots in ((-1, left, ((0, 0), (1, 1))), (1, right, ((cols - 2, 6), (cols - 1, 7)))):
            total, count = None, None
            for j, place in spots:
                mask = masks[side, j, shift]
                term = buf[:, place, :] * mask
                total = term if total is None else total + term
                count = mask if count is None else count + mask
            row += [total, jnp.broadcast_to(count, (rows, LANES))]
        parts.append(jnp.concatenate(row, axis=1))
    stacked = jnp.concatenate(parts, axis=0)
    r = lax.broadcasted_iota(jnp.int32, (rows, 3 * rows), 0)
    k = lax.broadcasted_iota(jnp.int32, (rows, 3 * rows), 1)
    pick = ((k % rows) // 2 + k // rows == r).astype(F32)
    both = dot(pick, stacked, lax.Precision.HIGHEST)
    left_out[...] = both[:, : length + LANES]
    right_out[...] = both[:, length + LANES :]


def bin_kernel(traces, steps, sums, keys, counts):
    rows, cols, length = traces.shape
    bins = cols // 2
    wide = pl.cdiv(cols, LANES) * LANES
    tall = pl.cdiv(3 * bins, 16) * 16
    column = lax.broadcasted_iota(jnp.int32, (rows, cols), 1) // 2 + steps[1]
    inside = (column >= 0) & (column < bins)
    key = jnp.where(inside, column + (steps[0] + 1) * bins, -1)
    keys[...] = jnp.concatenate([key, jnp.full((rows, wide - cols), -1, jnp.int32)], axis=1)
    sums[...] = jnp.zeros(sums.shape, F32)
    counts[...] = jnp.zeros(counts.shape, F32)
    slot = lax.broadcasted_iota(jnp.int32, (tall, wide), 0)
    pad = jnp.zeros((wide - cols, length), BF16)

    def body(a, _):
        total, count = None, None
        for p in (0, 1):
            i = 2 * a + p
            hot = jnp.where(slot == keys[pl.ds(i, 1), :], 1.0, 0.0).astype(F32)
            for c in range(wide // LANES):
                piece = hot[:, c * LANES : (c + 1) * LANES]
                count = piece if count is None else count + piece
            hot = hot.astype(BF16)
            for part in split(traces[i]):
                term = dot(hot, jnp.concatenate([part, pad], axis=0))
                total = term if total is None else total + term
        for s in range(3):
            sums[a + s, :, :length] += total[s * bins : (s + 1) * bins]
            counts[a + s] += count[s * bins : (s + 1) * bins]
        return 0

    lax.fori_loop(0, rows // 2, body, 0)
    for r in range(rows // 2 + 2):
        whole = jnp.sum(counts[r], axis=1, keepdims=True)
        sums[r, :, length:] = jnp.broadcast_to(whole, (bins, LANES))


def rightward(il, ta):
    return (il + ta) % 2 == 0


def edges(plane, length, lane0, right):
    if right:
        return pltpu.roll(plane[:, length - LANES : length], (lane0 + REACH) % LANES, 1)
    return pltpu.roll(plane[:, :LANES], lane0, 1) if lane0 else plane[:, :LANES]


def join_xl_kernel(sums_in, from_left, from_right, sums, payload, mine):
    rows, bins, width = sums.shape
    length = width - LANES
    inner = rows - 2
    xl, il, ta = lax.axis_index("xl"), lax.axis_index("il"), lax.axis_index("ta")
    has_left = xl > 0
    has_right = xl < lax.axis_size("xl") - 1
    sub = lax.broadcasted_iota(jnp.int32, (8, width), 0)
    for r in range(rows):
        gain = jnp.where((sub == 0) & has_left, jnp.broadcast_to(from_left[r : r + 1, :], (8, width)), 0.0)
        sums[r, 0:8, :] = sums_in[r, 0:8, :] + gain
        gain = jnp.where((sub == 7) & has_right, jnp.broadcast_to(from_right[r : r + 1, :], (8, width)), 0.0)
        sums[r, bins - 8 : bins, :] = sums_in[r, bins - 8 : bins, :] + gain
    lane = lax.broadcasted_iota(jnp.int32, (bins, LANES), 1)
    first = jnp.zeros((bins, LANES), F32)
    last = jnp.zeros((bins, LANES), F32)
    for b in range(inner):
        here = lane // REACH == b
        first = jnp.where(here, edges(sums[b + 1], length, b * REACH, False), first)
        last = jnp.where(here, edges(sums[b + 1], length, b * REACH, True), last)
    right = rightward(il, ta)
    payload[:, :width] = sums[jnp.where(il == 0, rows - 1, 0)]
    payload[:, width:] = jnp.where(right, first, last)
    mine[...] = jnp.where(right, last, first)


def join_il_kernel(payload, mine, got, out):
    bins, width = payload.shape
    width -= LANES
    length = width - LANES
    il, ta = lax.axis_index("il"), lax.axis_index("ta")
    right = rightward(il, ta)
    low = il == 0
    lane = lax.broadcasted_iota(jnp.int32, (bins, LANES), 1)
    other = got[:, width:]
    own = mine[...]
    near = jnp.where(low, own, other)
    far = pltpu.roll(jnp.where(low, other, own), LANES // 2, 1)
    chip = jnp.where(lane < LANES // 2, near, far)
    up = jnp.where(low, got[:, :length], payload[:, :length])
    down = jnp.where(low, payload[:, :length], got[:, :length])
    for plane, lane0 in ((up, LANES // 2 - REACH), (down, LANES // 2)):
        edge = jnp.where(right, edges(plane, length, lane0, True), edges(plane, length, lane0, False))
        chip = chip + jnp.where(lane // REACH == lane0 // REACH, edge, 0.0)
    out[...] = chip


def resampled(planes, table_h, table_l):
    count, bins, width = planes.shape
    length = width - LANES
    scale = 1.0 / jnp.maximum(planes[:, :, length:], 1.0)
    values = planes[:, :, :length] * jnp.concatenate([scale] * (length // LANES), axis=2)
    high, low = split(values.reshape(count * bins, length))
    out = dot(high, table_h) + dot(low, table_h) + dot(high, table_l)
    return out.reshape(count, bins, -1)


def resample_inner_kernel(sums, table_h, table_l, out):
    rows = sums.shape[0]
    out[...] = resampled(sums[2 : rows - 2], table_h[...], table_l[...])


def resample_outer_kernel(sums, got, table_h, table_l, out, folds):
    rows, bins, width = sums.shape
    low = lax.axis_index("il") == 0
    rim = got[:, :width]
    first = sums[1] + jnp.where(low, 0.0, rim)
    last = sums[rows - 2] + jnp.where(low, rim, 0.0)
    folds[0] = first[:, width - LANES :]
    folds[1] = last[:, width - LANES :]
    out[...] = resampled(jnp.stack([first, last]), table_h[...], table_l[...])


def finish_kernel(sums, folds, inner, outer, own, other, table_h, table_l, out):
    rows, bins, width = sums.shape
    length = width - LANES
    count = rows - 2
    il, ta = lax.axis_index("il"), lax.axis_index("ta")
    right = rightward(il, ta)
    low = il == 0
    half = LANES // 2
    lane = lax.broadcasted_iota(jnp.int32, (bins, LANES), 1)
    after = jnp.where(right, own[...], other[...])
    before = jnp.where(right, other[...], own[...])
    after = jnp.where(ta < lax.axis_size("ta") - 1, after, 0.0)
    before = jnp.where(ta > 0, before, 0.0)
    before = jnp.where(low, before, pltpu.roll(before, half, 1))
    after = jnp.where(low, pltpu.roll(after, half, 1), after)
    both = jnp.where(lane < half, before, after)
    pieces = []
    for b in range(count):
        if b in (0, count - 1):
            fold = folds[0 if b == 0 else 1]
        else:
            fold = sums[b + 1, :, length:]
        moved = pltpu.roll(both, LANES - b * REACH, 1) if b else both
        pieces.append(moved * (1.0 / jnp.maximum(fold, 1.0)))
    high, low_part = split(jnp.concatenate(pieces, axis=0))
    fix = dot(high, table_h[...]) + dot(low_part, table_h[...]) + dot(high, table_l[...])
    for b in range(count):
        base = outer.at[0 if b == 0 else 1] if b in (0, count - 1) else inner.at[b - 1]
        part = fix[b * bins : (b + 1) * bins]
        out[b, :, :LANES] = base[:, :LANES] + part[:, :LANES]
        out[b, :, LANES : out.shape[2] - LANES] = base[:, LANES : out.shape[2] - LANES]
        out[b, :, out.shape[2] - LANES :] = base[:, out.shape[2] - LANES :] + part[:, LANES:]


def call(kernel, outs, scratch=(), in_specs=None, aliases={}):
    shapes = [jax.ShapeDtypeStruct(dims, F32) for dims in outs]
    more = {} if in_specs is None else {"in_specs": in_specs}
    return pl.pallas_call(
        kernel,
        out_shape=shapes,
        scratch_shapes=list(scratch),
        input_output_aliases=aliases,
        compiler_params=pltpu.CompilerParams(vmem_limit_bytes=24 << 20),
        **more,
    )


def shards(sizes, traces, bin_steps):
    n_il, n_xl, n_ta = sizes
    rows, cols, length = traces.shape
    half, bins = rows // 2, cols // 2
    width = length + LANES
    out_len = length * P_SIZE // Q
    main = split_table(main_table(length))
    edge = split_table(edge_table(length))
    vmem = pl.BlockSpec(memory_space=pltpu.VMEM)

    rim = call(
        rim_kernel,
        [(rows, width)] * 2,
        [pltpu.VMEM((rows, 8, length), F32)] * 2 + [pltpu.SemaphoreType.DMA((2,))],
        [pl.BlockSpec(memory_space=pl.ANY), vmem],
    )
    to_left, to_right = rim(traces, bin_steps)
    up = [(i, (i + 1) % n_xl) for i in range(n_xl)]
    down = [(j, i) for i, j in up]
    from_left = lax.ppermute(to_right, "xl", up)
    from_right = lax.ppermute(to_left, "xl", down)

    wide = pl.cdiv(cols, LANES) * LANES
    (sums,) = call(
        bin_kernel,
        [(half + 2, bins, width)],
        [pltpu.VMEM((rows, wide), jnp.int32), pltpu.VMEM((half + 2, bins, LANES), F32)],
    )(traces, bin_steps)
    sums, payload, mine = call(
        join_xl_kernel,
        [(half + 2, bins, width), (bins, width + LANES), (bins, LANES)],
        aliases={0: 0},
    )(sums, from_left, from_right)

    swap = [(0, 1), (1, 0)]
    got = lax.ppermute(payload, "il", swap)
    (inner,) = call(resample_inner_kernel, [(half - 2, bins, out_len)])(sums, *main)
    (chip,) = call(join_il_kernel, [(bins, LANES)])(payload, mine, got)

    trades = []
    for core in range(2):
        for t in range(core, n_ta - 1, 2):
            trades += [(core * n_ta + t, core * n_ta + t + 1), (core * n_ta + t + 1, core * n_ta + t)]
    own = lax.ppermute(chip, ("il", "ta"), trades)
    outer, folds = call(resample_outer_kernel, [(2, bins, out_len), (2, bins, LANES)])(sums, got, *main)
    other = lax.ppermute(own, "il", swap)
    (out,) = call(finish_kernel, [(half, bins, out_len)])(sums, folds, inner, outer, own, other, *edge)
    return out


def solution(mesh):
    sizes = tuple(mesh.shape[axis] for axis in ("il", "xl", "ta"))
    assert sizes[0] == 2
    return jax.shard_map(
        functools.partial(shards, sizes),
        mesh=mesh,
        in_specs=(P("il", "xl", "ta"), P(None, "il", "xl")),
        out_specs=P("il", "xl", "ta"),
        check_vma=False,
    )
```

```python
import functools

import jax
import jax.numpy as jnp
import numpy as np
from jax import lax
from jax.experimental import pallas as pl
from jax.experimental.pallas import tpu as pltpu
from jax.sharding import PartitionSpec as P


TAPS = 16
P_SIZE = 3
Q = 2
REACH = TAPS // 2
LANES = 128
F32 = jnp.float32
BF16 = jnp.bfloat16


def weight(x):
    inside = np.abs(x) < REACH
    return np.where(inside, np.sinc(x) * np.sinc(x / REACH), 0.0)


def split_table(table):
    high = table.astype(BF16)
    return high, (table - high.astype(np.float64)).astype(BF16)


def main_table(length):
    n = np.arange(length)[:, None]
    m = np.arange(length * P_SIZE // Q)[None, :]
    return weight((m * Q - n * P_SIZE) / P_SIZE)


def edge_table(length):
    out_len = length * P_SIZE // Q
    table = np.zeros((2, LANES, LANES))
    k = np.arange(REACH)[:, None]
    m = np.arange(LANES)[None, :]
    table[0, :REACH] = weight((m * Q - (k - REACH) * P_SIZE) / P_SIZE)
    m = m + out_len - LANES
    table[1, :REACH] = weight((m * Q - (length + k) * P_SIZE) / P_SIZE)
    return table


def split(values):
    high = values.astype(BF16)
    return high, (values - high.astype(F32)).astype(BF16)


def dot(a, b, precision=None):
    return jnp.dot(a, b, precision=precision, preferred_element_type=F32)


def rim_kernel(traces, steps_hbm, left_out, right_out, left, right, steps, sems):
    rows, cols, length = traces.shape
    copy_s = pltpu.make_async_copy(steps_hbm, steps, sems.at[2])
    copy_l = pltpu.make_async_copy(traces.at[:, 0:8, :], left, sems.at[0])
    copy_r = pltpu.make_async_copy(traces.at[:, cols - 8 : cols, :], right, sems.at[1])
    copy_s.start()
    copy_l.start()
    copy_r.start()
    copy_s.wait()
    step_il = steps[0]
    step_xl = steps[1]
    masks = {}
    for side, spots in ((-1, (0, 1)), (1, (cols - 2, cols - 1))):
        for j in spots:
            for shift in (-1, 0, 1):
                hit = (step_xl[:, j : j + 1] == side) & (step_il[:, j : j + 1] == shift)
                masks[side, j, shift] = hit.astype(F32)
    copy_l.wait()
    copy_r.wait()
    parts = []
    for shift in (-1, 0, 1):
        row = []
        for side, buf, spots in ((-1, left, ((0, 0), (1, 1))), (1, right, ((cols - 2, 6), (cols - 1, 7)))):
            total, count = None, None
            for j, place in spots:
                mask = masks[side, j, shift]
                term = buf[:, place, :] * mask
                total = term if total is None else total + term
                count = mask if count is None else count + mask
            row += [total, jnp.broadcast_to(count, (rows, LANES))]
        parts.append(jnp.concatenate(row, axis=1))
    stacked = jnp.concatenate(parts, axis=0)
    r = lax.broadcasted_iota(jnp.int32, (rows, 3 * rows), 0)
    k = lax.broadcasted_iota(jnp.int32, (rows, 3 * rows), 1)
    pick = ((k % rows) // 2 + k // rows == r).astype(F32)
    both = dot(pick, stacked, lax.Precision.HIGHEST)
    left_out[...] = both[:, : length + LANES]
    right_out[...] = both[:, length + LANES :]


def bin_kernel(traces, steps, *refs):
    tables, (sums, *copies), (keys, counts, sems) = refs[:4], refs[4:9], refs[9:]
    loads = [pltpu.make_async_copy(a, b, sems.at[n]) for n, (a, b) in enumerate(zip(tables, copies))]
    for load in loads:
        load.start()
    rows, cols, length = traces.shape
    bins = cols // 2
    wide = pl.cdiv(cols, LANES) * LANES
    tall = pl.cdiv(3 * bins, 16) * 16
    column = lax.broadcasted_iota(jnp.int32, (rows, cols), 1) // 2 + steps[1]
    inside = (column >= 0) & (column < bins)
    key = jnp.where(inside, column + (steps[0] + 1) * bins, -1)
    keys[...] = jnp.concatenate([key, jnp.full((rows, wide - cols), -1, jnp.int32)], axis=1)
    sums[...] = jnp.zeros(sums.shape, F32)
    counts[...] = jnp.zeros(counts.shape, F32)
    slot = lax.broadcasted_iota(jnp.int32, (tall, wide), 0)
    pad = jnp.zeros((wide - cols, length), BF16)

    def body(a, _):
        total, count = None, None
        for p in (0, 1):
            i = 2 * a + p
            hot = jnp.where(slot == keys[pl.ds(i, 1), :], 1.0, 0.0).astype(F32)
            for c in range(wide // LANES):
                piece = hot[:, c * LANES : (c + 1) * LANES]
                count = piece if count is None else count + piece
            hot = hot.astype(BF16)
            for part in split(traces[i]):
                term = dot(hot, jnp.concatenate([part, pad], axis=0))
                total = term if total is None else total + term
        for s in range(3):
            sums[a + s, :, :length] += total[s * bins : (s + 1) * bins]
            counts[a + s] += count[s * bins : (s + 1) * bins]
        return 0

    lax.fori_loop(0, rows // 2, body, 0)
    for r in range(rows // 2 + 2):
        whole = jnp.sum(counts[r], axis=1, keepdims=True)
        sums[r, :, length:] = jnp.broadcast_to(whole, (bins, LANES))
    for load in loads:
        load.wait()


def edges(plane, length, lane0, right):
    if right:
        return pltpu.roll(plane[:, length - LANES : length], (lane0 + REACH) % LANES, 1)
    return pltpu.roll(plane[:, :LANES], lane0, 1) if lane0 else plane[:, :LANES]


def join_xl_kernel(sums_in, from_left, from_right, sums, payload, mine):
    rows, bins, width = sums.shape
    length = width - LANES
    inner = rows - 2
    xl, il = lax.axis_index("xl"), lax.axis_index("il")
    has_left = xl > 0
    has_right = xl < lax.axis_size("xl") - 1
    sub = lax.broadcasted_iota(jnp.int32, (8, width), 0)
    for r in range(rows):
        gain = jnp.where((sub == 0) & has_left, jnp.broadcast_to(from_left[r : r + 1, :], (8, width)), 0.0)
        sums[r, 0:8, :] = sums_in[r, 0:8, :] + gain
        gain = jnp.where((sub == 7) & has_right, jnp.broadcast_to(from_right[r : r + 1, :], (8, width)), 0.0)
        sums[r, bins - 8 : bins, :] = sums_in[r, bins - 8 : bins, :] + gain
    lane = lax.broadcasted_iota(jnp.int32, (bins, LANES), 1)
    first = jnp.zeros((bins, LANES), F32)
    last = jnp.zeros((bins, LANES), F32)
    for b in range(inner):
        here = lane // REACH == b
        first = jnp.where(here, edges(sums[b + 1], length, b * REACH, False), first)
        last = jnp.where(here, edges(sums[b + 1], length, b * REACH, True), last)
    low = il == 0
    payload[:, :width] = sums[jnp.where(low, rows - 1, 0)]
    payload[:, width:] = jnp.where(low, first, last)
    mine[...] = jnp.where(low, last, first)


def join_il_kernel(payload, mine, got, out):
    bins, width = payload.shape
    width -= LANES
    length = width - LANES
    low = lax.axis_index("il") == 0
    lane = lax.broadcasted_iota(jnp.int32, (bins, LANES), 1)
    other = got[:, width:]
    own = mine[...]
    near = jnp.where(low, own, other)
    far = pltpu.roll(jnp.where(low, other, own), LANES // 2, 1)
    chip = jnp.where(lane < LANES // 2, near, far)
    up = jnp.where(low, got[:, :length], payload[:, :length])
    down = jnp.where(low, payload[:, :length], got[:, :length])
    for plane, lane0 in ((up, LANES // 2 - REACH), (down, LANES // 2)):
        edge = jnp.where(low, edges(plane, length, lane0, True), edges(plane, length, lane0, False))
        chip = chip + jnp.where(lane // REACH == lane0 // REACH, edge, 0.0)
    out[...] = chip


def resampled(planes, table_h, table_l):
    count, bins, width = planes.shape
    length = width - LANES
    scale = 1.0 / jnp.maximum(planes[:, :, length:], 1.0)
    values = planes[:, :, :length] * jnp.concatenate([scale] * (length // LANES), axis=2)
    high, low = split(values.reshape(count * bins, length))
    out = dot(high, table_h) + dot(low, table_h) + dot(high, table_l)
    return out.reshape(count, bins, -1)


def write_middle(values, ends, middle, places, out, sem):
    ends[:, :, :LANES] = values[:, :, :LANES]
    ends[:, :, LANES:] = values[:, :, values.shape[2] - LANES :]
    middle[...] = values[:, :, LANES : values.shape[2] - LANES]
    copies = []
    for n, place in enumerate(places):
        copies.append(
            pltpu.make_async_copy(middle.at[n], out.at[place, :, LANES : out.shape[2] - LANES], sem.at[n])
        )
    for copy in copies:
        copy.start()
    for copy in copies:
        copy.wait()


def resample_inner_kernel(sums, table_h, table_l, out, ends, middle, sem):
    rows = sums.shape[0]
    values = resampled(sums[2 : rows - 2], table_h[...], table_l[...])
    write_middle(values, ends, middle, range(1, rows - 3), out, sem)


def resample_outer_kernel(out_in, sums, got, table_h, table_l, out, ends, folds, middle, sem):
    rows, _, width = sums.shape
    low = lax.axis_index("il") == 0
    rim = got[:, :width]
    first = sums[1] + jnp.where(low, 0.0, rim)
    last = sums[rows - 2] + jnp.where(low, rim, 0.0)
    folds[0] = first[:, width - LANES :]
    folds[1] = last[:, width - LANES :]
    values = resampled(jnp.stack([first, last]), table_h[...], table_l[...])
    write_middle(values, ends, middle, (0, rows - 3), out, sem)


def finish_kernel(own_side, out_in, sums, folds, inner, outer, got, table_h, table_l, out, piece, sem):
    rows, bins, width = sums.shape
    length = width - LANES
    count = rows - 2
    il, ta = lax.axis_index("il"), lax.axis_index("ta")
    low = il == 0
    half = LANES // 2
    before = low if own_side else ~low
    there = jnp.where(before, ta > 0, ta < lax.axis_size("ta") - 1)
    values = jnp.where(there, got[...], 0.0)
    values = jnp.where(low, values, pltpu.roll(values, half, 1))
    pieces = []
    for b in range(count):
        if b in (0, count - 1):
            fold = folds[0 if b == 0 else 1]
        else:
            fold = sums[b + 1, :, length:]
        moved = pltpu.roll(values, LANES - b * REACH, 1) if b else values
        pieces.append(moved * (1.0 / jnp.maximum(fold, 1.0)))
    high, low_part = split(jnp.concatenate(pieces, axis=0))
    side = jnp.where(before, 0, 1)
    start_h, start_l = table_h[side], table_l[side]
    fix = dot(high, start_h) + dot(low_part, start_h) + dot(high, start_l)
    start = pl.multiple_of(jnp.where(before, 0, out.shape[2] - LANES), LANES)
    copies = []
    for b in range(count):
        ends = outer.at[0 if b == 0 else 1] if b in (0, count - 1) else inner.at[b - 1]
        end = jnp.where(before, ends[:, :LANES], ends[:, LANES:])
        piece[b] = end + fix[b * bins : (b + 1) * bins]
        copies.append(pltpu.make_async_copy(piece.at[b], out.at[b, :, pl.ds(start, LANES)], sem.at[b]))
        copies[-1].start()
    for copy in copies:
        copy.wait()


VMEM = pl.BlockSpec(memory_space=pltpu.VMEM)
HBM = pl.BlockSpec(memory_space=pltpu.HBM)


def call(kernel, ins, outs, scratch=(), aliases={}):
    def run(*args):
        return pl.pallas_call(
            kernel,
            in_specs=ins,
            out_specs=[spec for spec, _ in outs],
            out_shape=[shape for _, shape in outs],
            scratch_shapes=list(scratch),
            input_output_aliases=aliases,
            compiler_params=pltpu.CompilerParams(vmem_limit_bytes=24 << 20),
        )(*args)

    return run


def in_hbm(values):
    return pltpu.with_memory_space_constraint(values, pltpu.HBM)


def vmem(*dims, kind=F32):
    return VMEM, jax.ShapeDtypeStruct(dims, kind)


def shards(sizes, traces, bin_steps):
    return steps_of(sizes, traces, bin_steps)


def steps_of(sizes, traces, bin_steps):
    _, n_xl, n_ta = sizes
    rows, cols, length = traces.shape
    half, bins = rows // 2, cols // 2
    width = length + LANES
    out_len = length * P_SIZE // Q
    main = split_table(main_table(length))
    edge = split_table(edge_table(length))
    dma = pltpu.SemaphoreType.DMA

    to_left, to_right = call(
        rim_kernel,
        [HBM, HBM],
        [vmem(rows, width)] * 2,
        [pltpu.VMEM((rows, 8, length), F32)] * 2 + [pltpu.VMEM(bin_steps.shape, jnp.int32), dma((3,))],
    )(in_hbm(traces), in_hbm(bin_steps))
    up = [(i, (i + 1) % n_xl) for i in range(n_xl)]
    down = [(j, i) for i, j in up]
    from_left = lax.ppermute(to_right, "xl", up)
    from_right = lax.ppermute(to_left, "xl", down)

    wide = pl.cdiv(cols, LANES) * LANES
    tables = (*main, *edge)
    sums, *tables = call(
        bin_kernel,
        [VMEM, VMEM] + [HBM] * 4,
        [vmem(half + 2, bins, width)] + [vmem(*t.shape, kind=BF16) for t in tables],
        [pltpu.VMEM((rows, wide), jnp.int32), pltpu.VMEM((half + 2, bins, LANES), F32), dma((4,))],
    )(traces, bin_steps, *[in_hbm(t) for t in tables])
    main, edge = tables[:2], tables[2:]
    sums, payload, mine = call(
        join_xl_kernel,
        [VMEM] * 3,
        [vmem(half + 2, bins, width), vmem(bins, width + LANES), vmem(bins, LANES)],
        aliases={0: 0},
    )(sums, from_left, from_right)

    swap = [(0, 1), (1, 0)]
    got = lax.ppermute(payload, "il", swap)
    whole = (HBM, jax.ShapeDtypeStruct((half, bins, out_len), F32))
    middle = out_len - 2 * LANES
    out, inner = call(
        resample_inner_kernel,
        [VMEM] * 3,
        [whole, vmem(half - 2, bins, 2 * LANES)],
        [pltpu.VMEM((half - 2, bins, middle), F32), dma((half - 2,))],
    )(sums, *main)
    (chip,) = call(join_il_kernel, [VMEM] * 3, [vmem(bins, LANES)])(payload, mine, got)

    trade = [(n_ta - 1, 2 * n_ta - 1), (n_ta, 0)]
    for t in range(n_ta - 1):
        trade += [(t, t + 1), (n_ta + t + 1, n_ta + t)]
    own = lax.ppermute(chip, ("il", "ta"), trade)
    out, outer, folds = call(
        resample_outer_kernel,
        [HBM] + [VMEM] * 4,
        [whole, vmem(2, bins, 2 * LANES), vmem(2, bins, LANES)],
        [pltpu.VMEM((2, bins, middle), F32), dma((2,))],
        {0: 0},
    )(out, sums, got, *main)
    other = lax.ppermute(own, "il", swap)
    for mine, halo in ((True, own), (False, other)):
        (out,) = call(
            functools.partial(finish_kernel, mine),
            [HBM] + [VMEM] * 7,
            [whole],
            [pltpu.VMEM((half, bins, LANES), F32), dma((half,))],
            {0: 0},
        )(out, sums, folds, inner, outer, halo, *edge)
    return out


def solution(mesh):
    sizes = tuple(mesh.shape[axis] for axis in ("il", "xl", "ta"))
    assert sizes[0] == 2
    return jax.shard_map(
        functools.partial(shards, sizes),
        mesh=mesh,
        in_specs=(P("il", "xl", "ta"), P(None, "il", "xl")),
        out_specs=P("il", "xl", "ta"),
        check_vma=False,
    )
```

```python
import functools

import jax
import jax.numpy as jnp
import numpy as np
from jax import lax
from jax.experimental import pallas as pl
from jax.experimental.pallas import tpu as pltpu
from jax.sharding import PartitionSpec as P


TAPS = 16
P_SIZE = 3
Q = 2
REACH = TAPS // 2
LANES = 128
F32 = jnp.float32
BF16 = jnp.bfloat16
SPREAD = 16


def weight(x):
    inside = np.abs(x) < REACH
    return np.where(inside, np.sinc(x) * np.sinc(x / REACH), 0.0)


def split_table(table):
    high = table.astype(BF16)
    return high, (table - high.astype(np.float64)).astype(BF16)


def main_table(length):
    n = np.arange(length)[:, None]
    m = np.arange(length * P_SIZE // Q)[None, :]
    return weight((m * Q - n * P_SIZE) / P_SIZE)


def edge_table(length, count):
    out_len = length * P_SIZE // Q
    assert count * REACH <= LANES // 2 and count * SPREAD <= LANES and REACH * P_SIZE <= SPREAD * Q
    table = np.zeros((LANES, 2 * LANES))
    k = np.arange(REACH)[:, None]
    m = np.arange(SPREAD)[None, :]
    before = weight((m * Q - (k - REACH) * P_SIZE) / P_SIZE)
    after = weight(((m + out_len - SPREAD) * Q - (length + k) * P_SIZE) / P_SIZE)
    for b in range(count):
        r, c = b * REACH, b * SPREAD
        table[r : r + REACH, c : c + SPREAD] = before
        r, c = r + LANES // 2, c + LANES
        table[r : r + REACH, c : c + SPREAD] = after
    return table


def split(values):
    high = values.astype(BF16)
    return high, (values - high.astype(F32)).astype(BF16)


def dot(a, b, precision=None):
    return jnp.dot(a, b, precision=precision, preferred_element_type=F32)


def rim_kernel(traces, steps_hbm, left_out, right_out, left, right, steps, sems):
    rows, cols, length = traces.shape
    copy_s = pltpu.make_async_copy(steps_hbm, steps, sems.at[2])
    copy_l = pltpu.make_async_copy(traces.at[:, 0:8, :], left, sems.at[0])
    copy_r = pltpu.make_async_copy(traces.at[:, cols - 8 : cols, :], right, sems.at[1])
    copy_s.start()
    copy_l.start()
    copy_r.start()
    copy_s.wait()
    step_il = steps[0]
    step_xl = steps[1]
    masks = {}
    for side, spots in ((-1, (0, 1)), (1, (cols - 2, cols - 1))):
        for j in spots:
            for shift in (-1, 0, 1):
                hit = (step_xl[:, j : j + 1] == side) & (step_il[:, j : j + 1] == shift)
                masks[side, j, shift] = hit.astype(F32)
    copy_l.wait()
    copy_r.wait()
    parts = []
    for shift in (-1, 0, 1):
        row = []
        for side, buf, spots in ((-1, left, ((0, 0), (1, 1))), (1, right, ((cols - 2, 6), (cols - 1, 7)))):
            total, count = None, None
            for j, place in spots:
                mask = masks[side, j, shift]
                term = buf[:, place, :] * mask
                total = term if total is None else total + term
                count = mask if count is None else count + mask
            row += [total, jnp.broadcast_to(count, (rows, LANES))]
        parts.append(jnp.concatenate(row, axis=1))
    stacked = jnp.concatenate(parts, axis=0)
    r = lax.broadcasted_iota(jnp.int32, (rows, 3 * rows), 0)
    k = lax.broadcasted_iota(jnp.int32, (rows, 3 * rows), 1)
    pick = ((k % rows) // 2 + k // rows == r).astype(F32)
    both = dot(pick, stacked, lax.Precision.HIGHEST)
    left_out[...] = both[:, : length + LANES]
    right_out[...] = both[:, length + LANES :]


def groups_of(cols):
    assert cols % 16 == 0 and cols >= LANES
    bins, most, out = cols // 2, LANES // 2 - 8, []
    for low in range(0, bins, most):
        high = min(bins, low + most)
        start = min(max((2 * low - 2) // 16 * 16, 0), cols - LANES)
        assert start <= max(2 * low - 2, 0) and min(2 * high + 2, cols) <= start + LANES
        out.append((low, high, start))
    return out


def bin_kernel(traces, steps, *refs):
    tables, (sums, first, last, *copies), (keys, counts, sems) = refs[:4], refs[4:11], refs[11:]
    loads = [pltpu.make_async_copy(a, b, sems.at[n]) for n, (a, b) in enumerate(zip(tables, copies))]
    for load in loads:
        load.start()
    rows, cols, length = traces.shape
    bins = cols // 2
    groups = groups_of(cols)
    column = lax.broadcasted_iota(jnp.int32, (rows, cols), 1) // 2 + steps[1]
    row = steps[0] + 1
    for g, (low, high, start) in enumerate(groups):
        here, there = column[:, start : start + LANES], row[:, start : start + LANES]
        inside = (here >= low) & (here < high)
        keys[g] = jnp.where(inside, there * (high - low) + here - low, -1)
    sums[...] = jnp.zeros(sums.shape, F32)
    counts[...] = jnp.zeros(counts.shape, F32)

    def body(a, _):
        parts = [split(traces[2 * a + p]) for p in (0, 1)]
        for g, (low, high, start) in enumerate(groups):
            n = high - low
            slot = lax.broadcasted_iota(jnp.int32, (pl.cdiv(3 * n, 16) * 16, LANES), 0)
            hots = [jnp.where(slot == keys[g, pl.ds(2 * a + p, 1), :], 1.0, 0.0).astype(F32) for p in (0, 1)]
            count = hots[0] + hots[1]
            hot = jnp.concatenate(hots, axis=1).astype(BF16)
            total = None
            for level in (0, 1):
                window = [parts[p][level][start : start + LANES] for p in (0, 1)]
                term = dot(hot, jnp.concatenate(window, axis=0))
                total = term if total is None else total + term
            for s in range(3):
                sums[a + s, low:high, :length] += total[s * n : (s + 1) * n]
                counts[a + s, low:high] += count[s * n : (s + 1) * n]
        return 0

    lax.fori_loop(0, rows // 2, body, 0, unroll=True)
    for r in range(rows // 2 + 2):
        whole = jnp.sum(counts[r], axis=1, keepdims=True)
        sums[r, :, length:] = jnp.broadcast_to(whole, (bins, LANES))
    lane = lax.broadcasted_iota(jnp.int32, (bins, LANES), 1)
    heads = jnp.zeros((bins, LANES), F32)
    tails = jnp.zeros((bins, LANES), F32)
    for b in range(rows // 2):
        here = lane // REACH == b
        heads = jnp.where(here, edges(sums[b + 1], length, b * REACH, False), heads)
        tails = jnp.where(here, edges(sums[b + 1], length, b * REACH, True), tails)
    first[...] = heads
    last[...] = tails
    for load in loads:
        load.wait()


def edges(plane, length, lane0, tail):
    if tail:
        return pltpu.roll(plane[:, length - LANES : length], (lane0 + REACH) % LANES, 1)
    return pltpu.roll(plane[:, :LANES], lane0, 1) if lane0 else plane[:, :LANES]


def join_xl_kernel(sums_in, from_left, from_right, first_in, last_in, sums, rim, first, last):
    rows, bins, width = sums.shape
    length = width - LANES
    xl = lax.axis_index("xl")
    low = lax.axis_index("il") == 0
    left = jnp.where(xl > 0, from_left[...], 0.0)
    right = jnp.where(xl < lax.axis_size("xl") - 1, from_right[...], 0.0)
    sub = lax.broadcasted_iota(jnp.int32, (8, width), 0)
    for values, place, base in ((left, 0, 0), (right, 7, bins - 8)):
        for r in range(rows):
            gain = jnp.where(sub == place, jnp.broadcast_to(values[r : r + 1], (8, width)), 0.0)
            sums[r, base : base + 8, :] = sums_in[r, base : base + 8, :] + gain
        lane = lax.broadcasted_iota(jnp.int32, (8, LANES), 1)
        tile = sub[:, :LANES]
        for old, new, tail in ((first_in, first, False), (last_in, last, True)):
            gain = jnp.zeros((8, LANES), F32)
            for b in range(rows - 2):
                moved = edges(values[b + 1 : b + 2], length, b * REACH, tail)
                gain = jnp.where(lane // REACH == b, jnp.broadcast_to(moved, (8, LANES)), gain)
            gain = jnp.where(tile == place, gain, 0.0)
            new[base : base + 8, :] = old[base : base + 8, :] + gain
    rim[...] = sums[jnp.where(low, rows - 1, 0)]


def join_il_kernel(first, last, got, one, two):
    bins, width = got.shape
    length = width - LANES
    low = lax.axis_index("il") == 0
    half = LANES // 2
    lane = lax.broadcasted_iota(jnp.int32, (bins, LANES), 1)
    values = []
    for old, tail in ((first, False), (last, True)):
        edge = edges(got[...], length, 0, tail)
        edge = jnp.where(low, pltpu.roll(edge, half - REACH, 1), edge)
        there = lane // REACH == jnp.where(low, half // REACH - 1, 0)
        values.append(packed(old[...] + jnp.where(there, edge, 0.0)))
    one[...] = jnp.where(low, values[1], values[0])
    two[...] = jnp.where(low, values[0], values[1])


def split_row(bins):
    return pl.cdiv(bins, 16) * 8


def packed(values):
    bins = values.shape[0]
    cut = split_row(bins)
    rest = jnp.concatenate([values[cut:], jnp.zeros((2 * cut - bins, LANES), F32)], axis=0)
    lane = lax.broadcasted_iota(jnp.int32, (cut, LANES), 1)
    return jnp.where(lane < LANES // 2, values[:cut], pltpu.roll(rest, LANES // 2, 1))


def unpacked(values, bins):
    return jnp.concatenate([values, pltpu.roll(values, LANES // 2, 1)[: bins - values.shape[0]]], axis=0)


def resampled(planes, table_h, table_l):
    count, bins, width = planes.shape
    length = width - LANES
    scale = 1.0 / jnp.maximum(planes[:, :, length:], 1.0)
    values = planes[:, :, :length] * jnp.concatenate([scale] * (length // LANES), axis=2)
    high, low = split(values.reshape(count * bins, length))
    out = dot(high, table_h) + dot(low, table_h) + dot(high, table_l)
    return out.reshape(count, bins, -1)


def write_middle(values, ends, middle, places, out, sem):
    ends[:, :, :LANES] = values[:, :, :LANES]
    ends[:, :, LANES:] = values[:, :, values.shape[2] - LANES :]
    middle[...] = values[:, :, LANES : values.shape[2] - LANES]
    copies = []
    for n, place in enumerate(places):
        copies.append(
            pltpu.make_async_copy(middle.at[n], out.at[place, :, LANES : out.shape[2] - LANES], sem.at[n])
        )
    for copy in copies:
        copy.start()
    for copy in copies:
        copy.wait()


def resample_inner_kernel(sums, table_h, table_l, out, ends, middle, sem):
    rows = sums.shape[0]
    values = resampled(sums[2 : rows - 2], table_h[...], table_l[...])
    write_middle(values, ends, middle, range(1, rows - 3), out, sem)


def resample_outer_kernel(out_in, sums, got, table_h, table_l, out, ends, folds, middle, sem):
    rows, _, width = sums.shape
    low = lax.axis_index("il") == 0
    rim = got[:, :width]
    first = sums[1] + jnp.where(low, 0.0, rim)
    last = sums[rows - 2] + jnp.where(low, rim, 0.0)
    folds[0] = first[:, width - LANES :]
    folds[1] = last[:, width - LANES :]
    values = resampled(jnp.stack([first, last]), table_h[...], table_l[...])
    write_middle(values, ends, middle, (0, rows - 3), out, sem)


def finish_kernel(out_in, sums, folds, inner, outer, one, two, table_h, table_l, out, ends, sem):
    rows, bins, width = sums.shape
    length = width - LANES
    count = rows - 2
    ta = lax.axis_index("ta")
    low = lax.axis_index("il") == 0
    half = LANES // 2
    before = jnp.where(low, one[...], two[...])
    after = jnp.where(low, two[...], one[...])
    before = unpacked(jnp.where(ta > 0, before, 0.0), bins)
    after = unpacked(jnp.where(ta < lax.axis_size("ta") - 1, after, 0.0), bins)
    lane = lax.broadcasted_iota(jnp.int32, (bins, LANES), 1)
    values = jnp.where(lane < half, before, pltpu.roll(after, half, 1))
    high, low_part = split(values)
    fix = dot(high, table_h[...]) + dot(low_part, table_h[...]) + dot(high, table_l[...])
    head, tail = fix[:, :LANES], fix[:, LANES:]
    copies = []
    for b in range(count):
        if b in (0, count - 1):
            base, fold = outer.at[0 if b == 0 else 1], folds[0 if b == 0 else 1]
        else:
            base, fold = inner.at[b - 1], sums[b + 1, :, length:]
        scale = 1.0 / jnp.maximum(fold, 1.0)
        moved = pltpu.roll(head, LANES - b * SPREAD, 1) if b else head
        ends[b, 0] = base[:, :LANES] + jnp.where(lane < SPREAD, moved, 0.0) * scale
        moved = pltpu.roll(tail, (2 * LANES - (b + 1) * SPREAD) % LANES, 1)
        ends[b, 1] = base[:, LANES:] + jnp.where(lane >= LANES - SPREAD, moved, 0.0) * scale
        for side, start in ((0, 0), (1, out.shape[2] - LANES)):
            copies.append(
                pltpu.make_async_copy(ends.at[b, side], out.at[b, :, start : start + LANES], sem.at[b, side])
            )
            copies[-1].start()
    for copy in copies:
        copy.wait()


VMEM = pl.BlockSpec(memory_space=pltpu.VMEM)
HBM = pl.BlockSpec(memory_space=pltpu.HBM)


def call(kernel, ins, outs, scratch=(), aliases={}):
    def run(*args):
        return pl.pallas_call(
            kernel,
            in_specs=ins,
            out_specs=[spec for spec, _ in outs],
            out_shape=[shape for _, shape in outs],
            scratch_shapes=list(scratch),
            input_output_aliases=aliases,
            compiler_params=pltpu.CompilerParams(vmem_limit_bytes=24 << 20),
        )(*args)

    return run


def in_hbm(values):
    return pltpu.with_memory_space_constraint(values, pltpu.HBM)


def vmem(*dims, kind=F32):
    return VMEM, jax.ShapeDtypeStruct(dims, kind)


def shards(sizes, traces, bin_steps):
    return steps_of(sizes, traces, bin_steps)


def steps_of(sizes, traces, bin_steps):
    _, n_xl, n_ta = sizes
    rows, cols, length = traces.shape
    half, bins = rows // 2, cols // 2
    width = length + LANES
    out_len = length * P_SIZE // Q
    main = split_table(main_table(length))
    edge = split_table(edge_table(length, half))
    dma = pltpu.SemaphoreType.DMA

    to_left, to_right = call(
        rim_kernel,
        [HBM, HBM],
        [vmem(rows, width)] * 2,
        [pltpu.VMEM((rows, 8, length), F32)] * 2 + [pltpu.VMEM(bin_steps.shape, jnp.int32), dma((3,))],
    )(in_hbm(traces), in_hbm(bin_steps))
    up = [(i, (i + 1) % n_xl) for i in range(n_xl)]
    down = [(j, i) for i, j in up]
    from_left = lax.ppermute(to_right, "xl", up)
    from_right = lax.ppermute(to_left, "xl", down)

    tables = (*main, *edge)
    sums, first, last, *tables = call(
        bin_kernel,
        [VMEM, VMEM] + [HBM] * 4,
        [vmem(half + 2, bins, width)] + [vmem(bins, LANES)] * 2 + [vmem(*t.shape, kind=BF16) for t in tables],
        [pltpu.VMEM((len(groups_of(cols)), rows, LANES), jnp.int32), pltpu.VMEM((half + 2, bins, LANES), F32), dma((4,))],
    )(traces, bin_steps, *[in_hbm(t) for t in tables])
    main, edge = tables[:2], tables[2:]
    sums, rim, first, last = call(
        join_xl_kernel,
        [VMEM] * 5,
        [vmem(half + 2, bins, width), vmem(bins, width)] + [vmem(bins, LANES)] * 2,
        aliases={0: 0, 3: 2, 4: 3},
    )(sums, from_left, from_right, first, last)

    swap = [(0, 1), (1, 0)]
    got = lax.ppermute(rim, "il", swap)
    whole = (HBM, jax.ShapeDtypeStruct((half, bins, out_len), F32))
    middle = out_len - 2 * LANES
    out, inner = call(
        resample_inner_kernel,
        [VMEM] * 3,
        [whole, vmem(half - 2, bins, 2 * LANES)],
        [pltpu.VMEM((half - 2, bins, middle), F32), dma((half - 2,))],
    )(sums, *main)
    one, two = call(join_il_kernel, [VMEM] * 3, [vmem(split_row(bins), LANES)] * 2)(first, last, got)

    trade = [(n_ta - 1, 2 * n_ta - 1), (n_ta, 0)]
    for t in range(n_ta - 1):
        trade += [(t, t + 1), (n_ta + t + 1, n_ta + t)]
    one = lax.ppermute(one, ("il", "ta"), trade)
    two = lax.ppermute(two, ("il", "ta"), [(j, i) for i, j in trade])
    out, outer, folds = call(
        resample_outer_kernel,
        [HBM] + [VMEM] * 4,
        [whole, vmem(2, bins, 2 * LANES), vmem(2, bins, LANES)],
        [pltpu.VMEM((2, bins, middle), F32), dma((2,))],
        {0: 0},
    )(out, sums, got, *main)
    (out,) = call(
        finish_kernel, [HBM] + [VMEM] * 8, [whole], [pltpu.VMEM((half, 2, bins, LANES), F32), dma((half, 2))], {0: 0}
    )(out, sums, folds, inner, outer, one, two, *edge)
    return out


def solution(mesh):
    sizes = tuple(mesh.shape[axis] for axis in ("il", "xl", "ta"))
    assert sizes[0] == 2
    return jax.shard_map(
        functools.partial(shards, sizes),
        mesh=mesh,
        in_specs=(P("il", "xl", "ta"), P(None, "il", "xl")),
        out_specs=P("il", "xl", "ta"),
        check_vma=False,
    )
```

```python
import functools

import jax
import jax.numpy as jnp
import numpy as np
from jax import lax
from jax.experimental import pallas as pl
from jax.experimental.pallas import tpu as pltpu
from jax.sharding import PartitionSpec as P


TAPS = 16
P_SIZE = 3
Q = 2
REACH = TAPS // 2
LANES = 128
F32 = jnp.float32
BF16 = jnp.bfloat16
SPREAD = 16


def weight(x):
    inside = np.abs(x) < REACH
    return np.where(inside, np.sinc(x) * np.sinc(x / REACH), 0.0)


def split_table(table):
    high = table.astype(BF16)
    return high, (table - high.astype(np.float64)).astype(BF16)


def main_table(length):
    n = np.arange(length)[:, None]
    m = np.arange(length * P_SIZE // Q)[None, :]
    return weight((m * Q - n * P_SIZE) / P_SIZE)


def edge_table(length, count):
    out_len = length * P_SIZE // Q
    assert count * REACH <= LANES // 2 and count * SPREAD <= LANES and REACH * P_SIZE <= SPREAD * Q
    table = np.zeros((2, LANES, LANES))
    k = np.arange(REACH)[:, None]
    m = np.arange(SPREAD)[None, :]
    before = weight((m * Q - (k - REACH) * P_SIZE) / P_SIZE)
    after = weight(((m + out_len - SPREAD) * Q - (length + k) * P_SIZE) / P_SIZE)
    for b in range(count):
        r, c = b * REACH, b * SPREAD
        table[0, r : r + REACH, c : c + SPREAD] = before
        table[1, r : r + REACH, c : c + SPREAD] = after
    return table


def split(values):
    high = values.astype(BF16)
    return high, (values - high.astype(F32)).astype(BF16)


def dot(a, b, precision=None):
    return jnp.dot(a, b, precision=precision, preferred_element_type=F32)


def rim_kernel(traces, steps_hbm, keep, give, left, right, steps, sems):
    rows, cols, length = traces.shape
    copies = (
        pltpu.make_async_copy(steps_hbm, steps, sems.at[2]),
        pltpu.make_async_copy(traces.at[:, 0:8, :], left, sems.at[0]),
        pltpu.make_async_copy(traces.at[:, cols - 8 : cols, :], right, sems.at[1]),
    )
    for copy in copies:
        copy.start(priority=1)
    low = lax.axis_index("il") == 0
    g = lax.broadcasted_iota(jnp.int32, (rows, 6 * rows), 0) + jnp.where(low, 1, 1 - rows // 2)
    k = lax.broadcasted_iota(jnp.int32, (rows, 6 * rows), 1) % (3 * rows)
    pick = ((k % rows) // 2 + k // rows == g).astype(F32).astype(BF16)
    copies[0].wait()
    step_il = steps[0]
    step_xl = steps[1]
    masks = {}
    for side, spots in ((-1, (0, 1)), (1, (cols - 2, cols - 1))):
        for j in spots:
            for shift in (-1, 0, 1):
                hit = (step_xl[:, j : j + 1] == side) & (step_il[:, j : j + 1] == shift)
                masks[side, j, shift] = hit.astype(F32)
    copies[1].wait()
    copies[2].wait()
    sides = []
    for side, buf, spots in ((-1, left, ((0, 0), (1, 1))), (1, right, ((cols - 2, 6), (cols - 1, 7)))):
        parts = []
        for shift in (-1, 0, 1):
            total, count = None, None
            for j, place in spots:
                mask = masks[side, j, shift]
                term = buf[:, place, :] * mask
                total = term if total is None else total + term
                count = mask if count is None else count + mask
            parts.append(jnp.concatenate([total, jnp.broadcast_to(count, (rows, LANES))], axis=1))
        sides.append(jnp.concatenate(parts, axis=0))
    both = dot(pick, jnp.concatenate(split(jnp.concatenate(sides, axis=1)), axis=0))
    to_left, to_right = both[:, : length + LANES], both[:, length + LANES :]
    keep[...] = jnp.where(low, to_right, to_left)
    give[...] = jnp.where(low, to_left, to_right)


def groups_of(cols):
    assert cols % 16 == 0 and cols >= LANES
    bins, most, out = cols // 2, LANES // 2 - 8, []
    for low in range(0, bins, most):
        high = min(bins, low + most)
        start = min(max((2 * low - 2) // 16 * 16, 0), cols - LANES)
        assert start <= max(2 * low - 2, 0) and min(2 * high + 2, cols) <= start + LANES
        out.append((low, high, start))
    return out


def bin_kernel(traces, steps, *refs):
    tables, (sums, first, last, *copies), (keys, counts, sems) = refs[:4], refs[4:11], refs[11:]
    loads = [pltpu.make_async_copy(a, b, sems.at[n]) for n, (a, b) in enumerate(zip(tables, copies))]
    for load in loads:
        load.start()
    rows, cols, length = traces.shape
    bins = cols // 2
    groups = groups_of(cols)
    column = lax.broadcasted_iota(jnp.int32, (rows, cols), 1) // 2 + steps[1]
    row = steps[0] + 1
    for g, (low, high, start) in enumerate(groups):
        here, there = column[:, start : start + LANES], row[:, start : start + LANES]
        inside = (here >= low) & (here < high)
        keys[g] = jnp.where(inside, there * (high - low) + here - low, -1)
    sums[...] = jnp.zeros(sums.shape, F32)
    counts[...] = jnp.zeros(counts.shape, F32)

    def body(a, _):
        parts = [split(traces[2 * a + p]) for p in (0, 1)]
        for g, (low, high, start) in enumerate(groups):
            n = high - low
            slot = lax.broadcasted_iota(jnp.int32, (pl.cdiv(3 * n, 16) * 16, LANES), 0)
            hots = [jnp.where(slot == keys[g, pl.ds(2 * a + p, 1), :], 1.0, 0.0).astype(F32) for p in (0, 1)]
            count = hots[0] + hots[1]
            hot = jnp.concatenate(hots, axis=1).astype(BF16)
            total = None
            for level in (0, 1):
                window = [parts[p][level][start : start + LANES] for p in (0, 1)]
                term = dot(hot, jnp.concatenate(window, axis=0))
                total = term if total is None else total + term
            for s in range(3):
                sums[a + s, low:high, :length] += total[s * n : (s + 1) * n]
                counts[a + s, low:high] += count[s * n : (s + 1) * n]
        return 0

    lax.fori_loop(0, rows // 2, body, 0, unroll=True)
    for r in range(rows // 2 + 2):
        whole = jnp.sum(counts[r], axis=1, keepdims=True)
        sums[r, :, length:] = jnp.broadcast_to(whole, (bins, LANES))
    lane = lax.broadcasted_iota(jnp.int32, (bins, LANES), 1)
    heads = jnp.zeros((bins, LANES), F32)
    tails = jnp.zeros((bins, LANES), F32)
    for b in range(rows // 2):
        here = lane // REACH == b
        heads = jnp.where(here, edges(sums[b + 1], length, b * REACH, False), heads)
        tails = jnp.where(here, edges(sums[b + 1], length, b * REACH, True), tails)
    first[...] = heads
    last[...] = tails
    for load in loads:
        load.wait()


def edges(plane, length, lane0, tail):
    if tail:
        return pltpu.roll(plane[:, length - LANES : length], (lane0 + REACH) % LANES, 1)
    return pltpu.roll(plane[:, :LANES], lane0, 1) if lane0 else plane[:, :LANES]


def add_column(values, at_start, sums, first, last):
    rows, bins, width = sums.shape
    length = width - LANES
    sub = lax.broadcasted_iota(jnp.int32, (8, width), 0)
    place = jnp.where(at_start, 0, 7)
    base = pl.multiple_of(jnp.where(at_start, 0, bins - 8), 8)
    there = sub == place
    for b in range(rows - 2):
        gain = jnp.where(there, jnp.broadcast_to(values[b : b + 1], (8, width)), 0.0)
        sums[b + 1, pl.ds(base, 8), :] += gain
    lane = lax.broadcasted_iota(jnp.int32, (8, LANES), 1)
    for edge, tail in ((first, False), (last, True)):
        gain = jnp.zeros((8, LANES), F32)
        for b in range(rows - 2):
            row = edges(values[b : b + 1], length, b * REACH, tail)
            gain = jnp.where(lane // REACH == b, jnp.broadcast_to(row, (8, LANES)), gain)
        edge[pl.ds(base, 8), :] += jnp.where(there[:, :LANES], gain, 0.0)


def join_xl_kernel(sums_in, got, first_in, last_in, sums, payload, first, last):
    rows, bins, _ = sums.shape
    xl = lax.axis_index("xl")
    low = lax.axis_index("il") == 0
    there = jnp.where(low, xl > 0, xl < lax.axis_size("xl") - 1)
    count = rows - 2
    values = jnp.where(there, got[...], 0.0)
    payload[:bins, :] = sums[jnp.where(low, rows - 1, 0)]
    payload[bins:, :] = jnp.where(low, values[count:], values[:count])
    add_column(jnp.where(low, values[:count], values[count:]), low, sums, first, last)


def join_il_kernel(sums_in, first_in, last_in, got, sums, first, last, one, two):
    rows, bins, width = sums.shape
    length = width - LANES
    low = lax.axis_index("il") == 0
    half = LANES // 2
    add_column(got[bins:], ~low, sums, first, last)
    rim = got[:bins]
    sums[jnp.where(low, rows - 2, 1)] += rim
    lane = lax.broadcasted_iota(jnp.int32, (bins, LANES), 1)
    values = []
    for old, tail in ((first, False), (last, True)):
        edge = edges(rim, length, 0, tail)
        edge = jnp.where(low, pltpu.roll(edge, half - REACH, 1), edge)
        there = lane // REACH == jnp.where(low, half // REACH - 1, 0)
        values.append(packed(old[...] + jnp.where(there, edge, 0.0)))
    one[...] = jnp.where(low, values[1], values[0])
    two[...] = jnp.where(low, values[0], values[1])


def split_row(bins):
    return pl.cdiv(bins, 16) * 8


def packed(values):
    bins = values.shape[0]
    cut = split_row(bins)
    rest = jnp.concatenate([values[cut:], jnp.zeros((2 * cut - bins, LANES), F32)], axis=0)
    lane = lax.broadcasted_iota(jnp.int32, (cut, LANES), 1)
    return jnp.where(lane < LANES // 2, values[:cut], pltpu.roll(rest, LANES // 2, 1))


def unpacked(values, bins):
    return jnp.concatenate([values, pltpu.roll(values, LANES // 2, 1)[: bins - values.shape[0]]], axis=0)


def resample_kernel(sums, table_h, table_l, out, ends, scales, middle, sem):
    rows, bins, width = sums.shape
    length = width - LANES
    count = rows - 2
    out_len = out.shape[2]
    step = 2
    copies = []
    for start in range(0, count, step):
        planes = sums[start + 1 : start + 1 + step]
        scale = 1.0 / jnp.maximum(planes[:, :, length:], 1.0)
        scales[start : start + step] = scale
        values = planes[:, :, :length] * jnp.concatenate([scale] * (length // LANES), axis=2)
        high, low = split(values.reshape(step * bins, length))
        got = dot(high, table_h[...]) + dot(low, table_h[...]) + dot(high, table_l[...])
        got = got.reshape(step, bins, out_len)
        middle[start : start + step] = got[:, :, LANES : out_len - LANES]
        copies.append(
            pltpu.make_async_copy(
                middle.at[start : start + step],
                out.at[start : start + step, :, LANES : out_len - LANES],
                sem.at[start // step],
            )
        )
        copies[-1].start()
        ends[start : start + step, :, :LANES] = got[:, :, :LANES]
        ends[start : start + step, :, LANES:] = got[:, :, out_len - LANES :]
    for copy in copies:
        copy.wait()


def finish_kernel(first_trade, out_in, ends, scales, got, table_h, table_l, out, piece, sem):
    count, bins, _ = ends.shape
    ta = lax.axis_index("ta")
    low = lax.axis_index("il") == 0
    before = low if first_trade else ~low
    there = jnp.where(before, ta > 0, ta < lax.axis_size("ta") - 1)
    values = unpacked(jnp.where(there, got[...], 0.0), bins)
    high, low_part = split(values)
    side = jnp.where(before, 0, 1)
    start_h, start_l = table_h[side], table_l[side]
    fix = dot(high, start_h) + dot(low_part, start_h) + dot(high, start_l)
    fix = jnp.where(before, fix, pltpu.roll(fix, LANES - SPREAD, 1))
    lane = lax.broadcasted_iota(jnp.int32, (bins, LANES), 1)
    here = jnp.where(before, lane, LANES - 1 - lane) < SPREAD
    start = pl.multiple_of(jnp.where(before, 0, out.shape[2] - LANES), LANES)
    copies = []
    for b in range(count):
        base = jnp.where(before, ends[b, :, :LANES], ends[b, :, LANES:])
        moved = pltpu.roll(fix, LANES - b * SPREAD, 1) if b else fix
        piece[b] = base + jnp.where(here, moved, 0.0) * scales[b]
        copies.append(pltpu.make_async_copy(piece.at[b], out.at[b, :, pl.ds(start, LANES)], sem.at[b]))
        copies[-1].start()
    for copy in copies:
        copy.wait()


VMEM = pl.BlockSpec(memory_space=pltpu.VMEM)
HBM = pl.BlockSpec(memory_space=pltpu.HBM)


def call(kernel, ins, outs, scratch=(), aliases={}):
    def run(*args):
        return pl.pallas_call(
            kernel,
            in_specs=ins,
            out_specs=[spec for spec, _ in outs],
            out_shape=[shape for _, shape in outs],
            scratch_shapes=list(scratch),
            input_output_aliases=aliases,
            compiler_params=pltpu.CompilerParams(vmem_limit_bytes=24 << 20),
        )(*args)

    return run


def in_hbm(values):
    return pltpu.with_memory_space_constraint(values, pltpu.HBM)


def vmem(*dims, kind=F32):
    return VMEM, jax.ShapeDtypeStruct(dims, kind)


def shards(sizes, traces, bin_steps):
    return steps_of(sizes, traces, bin_steps)


def steps_of(sizes, traces, bin_steps):
    _, n_xl, n_ta = sizes
    rows, cols, length = traces.shape
    half, bins = rows // 2, cols // 2
    width = length + LANES
    out_len = length * P_SIZE // Q
    main = split_table(main_table(length))
    edge = split_table(edge_table(length, half))
    dma = pltpu.SemaphoreType.DMA

    keep, give = call(
        rim_kernel,
        [HBM, HBM],
        [vmem(rows, width)] * 2,
        [pltpu.VMEM((rows, 8, length), F32)] * 2 + [pltpu.VMEM(bin_steps.shape, jnp.int32), dma((3,))],
    )(in_hbm(traces), in_hbm(bin_steps))
    swap = [(0, 1), (1, 0)]
    chip_rims = keep + lax.ppermute(give, "il", swap)
    came = lax.ppermute(chip_rims, ("il", "xl"), turning(n_xl))

    tables = (*main, *edge)
    sums, first, last, *tables = call(
        bin_kernel,
        [VMEM, VMEM] + [HBM] * 4,
        [vmem(half + 2, bins, width)] + [vmem(bins, LANES)] * 2 + [vmem(*t.shape, kind=BF16) for t in tables],
        [pltpu.VMEM((len(groups_of(cols)), rows, LANES), jnp.int32), pltpu.VMEM((half + 2, bins, LANES), F32), dma((4,))],
    )(traces, bin_steps, *[in_hbm(t) for t in tables])
    main, edge = tables[:2], tables[2:]
    sums, payload, first, last = call(
        join_xl_kernel,
        [VMEM] * 4,
        [vmem(half + 2, bins, width), vmem(bins + half, width)] + [vmem(bins, LANES)] * 2,
        aliases={0: 0, 2: 2, 3: 3},
    )(sums, came, first, last)
    got = lax.ppermute(payload, "il", swap)
    sums, first, last, one, two = call(
        join_il_kernel,
        [VMEM] * 4,
        [vmem(half + 2, bins, width)] + [vmem(bins, LANES)] * 2 + [vmem(split_row(bins), LANES)] * 2,
        aliases={0: 0, 1: 1, 2: 2},
    )(sums, first, last, got)
    one = lax.ppermute(one, ("il", "ta"), turning(n_ta))
    two = lax.ppermute(two, ("il", "ta"), [(j, i) for i, j in turning(n_ta)])

    whole = (HBM, jax.ShapeDtypeStruct((half, bins, out_len), F32))
    out, ends, scales = call(
        resample_kernel,
        [VMEM] * 3,
        [whole, vmem(half, bins, 2 * LANES), vmem(half, bins, LANES)],
        [pltpu.VMEM((half, bins, out_len - 2 * LANES), F32), dma((half // 2,))],
    )(sums, *main)
    for first_trade, halo in ((True, one), (False, two)):
        (out,) = call(
            functools.partial(finish_kernel, first_trade),
            [HBM] + [VMEM] * 5,
            [whole],
            [pltpu.VMEM((half, bins, LANES), F32), dma((half,))],
            {0: 0},
        )(out, ends, scales, halo, *edge)
    return out


def turning(count):
    pairs = [(count - 1, 2 * count - 1), (count, 0)]
    for i in range(count - 1):
        pairs += [(i, i + 1), (count + i + 1, count + i)]
    return pairs


def solution(mesh):
    sizes = tuple(mesh.shape[axis] for axis in ("il", "xl", "ta"))
    assert sizes[0] == 2
    return jax.shard_map(
        functools.partial(shards, sizes),
        mesh=mesh,
        in_specs=(P("il", "xl", "ta"), P(None, "il", "xl")),
        out_specs=P("il", "xl", "ta"),
        check_vma=False,
    )
```

```python
import functools

import jax
import jax.numpy as jnp
import numpy as np
from jax import lax
from jax.experimental import pallas as pl
from jax.experimental.pallas import tpu as pltpu
from jax.sharding import PartitionSpec as P


TAPS = 16
P_SIZE = 3
Q = 2
REACH = TAPS // 2
LANES = 128
F32 = jnp.float32
BF16 = jnp.bfloat16
SPREAD = 16


def weight(x):
    inside = np.abs(x) < REACH
    return np.where(inside, np.sinc(x) * np.sinc(x / REACH), 0.0)


def split_table(table):
    high = table.astype(BF16)
    return high, (table - high.astype(np.float64)).astype(BF16)


def main_table(length):
    n = np.arange(length)[:, None]
    m = np.arange(length * P_SIZE // Q)[None, :]
    return weight((m * Q - n * P_SIZE) / P_SIZE)


def edge_table(length, count):
    out_len = length * P_SIZE // Q
    assert count * REACH <= LANES // 2 and count * SPREAD <= LANES and REACH * P_SIZE <= SPREAD * Q
    table = np.zeros((2, LANES, LANES))
    k = np.arange(REACH)[:, None]
    m = np.arange(SPREAD)[None, :]
    before = weight((m * Q - (k - REACH) * P_SIZE) / P_SIZE)
    after = weight(((m + out_len - SPREAD) * Q - (length + k) * P_SIZE) / P_SIZE)
    for b in range(count):
        r, c = b * REACH, b * SPREAD
        table[0, r : r + REACH, c : c + SPREAD] = before
        table[1, r : r + REACH, c : c + SPREAD] = after
    return table


def split(values):
    high = values.astype(BF16)
    return high, (values - high.astype(F32)).astype(BF16)


def dot(a, b, precision=None):
    return jnp.dot(a, b, precision=precision, preferred_element_type=F32)


def sends_up():
    return (lax.axis_index("il") + lax.axis_index("xl")) % 2 == 0


def gets():
    xl, last = lax.axis_index("xl"), lax.axis_size("xl") - 1
    low = lax.axis_index("il") == 0
    end = (xl == 0) | (xl == last)
    return jnp.where(end, xl == 0, sends_up()), ~(end & low)


def other_at_start():
    xl, last = lax.axis_index("xl"), lax.axis_size("xl") - 1
    end = (xl == 0) | (xl == last)
    return jnp.where(end, xl == last, sends_up())


def paired(count):
    assert count % 2 == 0 and count > 2
    last = count - 1
    target = {i: i ^ 1 for i in range(count)}
    for i in range(1, last, 2):
        target[count + i], target[count + i + 1] = count + i + 1, count + i
    for end in (0, last):
        target[end ^ 1] = count + end
        target[count + end] = end
    return sorted(target.items())


def rim_kernel(traces, steps_hbm, keep, give, left, right, steps, sems):
    rows, cols, length = traces.shape
    copies = (
        pltpu.make_async_copy(steps_hbm, steps, sems.at[2]),
        pltpu.make_async_copy(traces.at[:, 0:8, :], left, sems.at[0]),
        pltpu.make_async_copy(traces.at[:, cols - 8 : cols, :], right, sems.at[1]),
    )
    for copy in copies:
        copy.start(priority=1)
    low = lax.axis_index("il") == 0
    up = sends_up()
    g = lax.broadcasted_iota(jnp.int32, (rows, 6 * rows), 0) + jnp.where(low, 1, 1 - rows // 2)
    k = lax.broadcasted_iota(jnp.int32, (rows, 6 * rows), 1) % (3 * rows)
    pick = ((k % rows) // 2 + k // rows == g).astype(F32).astype(BF16)
    copies[0].wait()
    step_il = steps[0]
    step_xl = steps[1]
    masks = {}
    for side, spots in ((-1, (0, 1)), (1, (cols - 2, cols - 1))):
        for j in spots:
            for shift in (-1, 0, 1):
                hit = (step_xl[:, j : j + 1] == side) & (step_il[:, j : j + 1] == shift)
                masks[side, j, shift] = hit.astype(F32)
    copies[1].wait()
    copies[2].wait()
    sides = []
    for side, buf, spots in ((-1, left, ((0, 0), (1, 1))), (1, right, ((cols - 2, 6), (cols - 1, 7)))):
        parts = []
        for shift in (-1, 0, 1):
            total, count = None, None
            for j, place in spots:
                mask = masks[side, j, shift]
                term = buf[:, place, :] * mask
                total = term if total is None else total + term
                count = mask if count is None else count + mask
            parts.append(jnp.concatenate([total, jnp.broadcast_to(count, (rows, LANES))], axis=1))
        sides.append(jnp.concatenate(parts, axis=0))
    both = dot(pick, jnp.concatenate(split(jnp.concatenate(sides, axis=1)), axis=0))
    to_left, to_right = both[:, : length + LANES], both[:, length + LANES :]
    keep[...] = jnp.where(up, to_right, to_left)
    give[...] = jnp.where(up, to_left, to_right)


def groups_of(cols):
    assert cols % 16 == 0 and cols >= LANES
    bins, most, out = cols // 2, LANES // 2 - 8, []
    for low in range(0, bins, most):
        high = min(bins, low + most)
        start = min(max((2 * low - 2) // 16 * 16, 0), cols - LANES)
        assert start <= max(2 * low - 2, 0) and min(2 * high + 2, cols) <= start + LANES
        out.append((low, high, start))
    return out


def bin_kernel(traces, steps, *refs):
    tables, (sums, *copies), (keys, counts, sems) = refs[:4], refs[4:9], refs[9:]
    loads = [pltpu.make_async_copy(a, b, sems.at[n]) for n, (a, b) in enumerate(zip(tables, copies))]
    for load in loads:
        load.start()
    rows, cols, length = traces.shape
    bins = cols // 2
    groups = groups_of(cols)
    column = lax.broadcasted_iota(jnp.int32, (rows, cols), 1) // 2 + steps[1]
    row = steps[0] + 1
    for g, (low, high, start) in enumerate(groups):
        here, there = column[:, start : start + LANES], row[:, start : start + LANES]
        inside = (here >= low) & (here < high)
        keys[g] = jnp.where(inside, there * (high - low) + here - low, -1)
    for a in range(rows // 2):
        parts = [split(traces[2 * a + p]) for p in (0, 1)]
        for g, (low, high, start) in enumerate(groups):
            n = high - low
            slot = lax.broadcasted_iota(jnp.int32, (pl.cdiv(3 * n, 16) * 16, LANES), 0)
            hots = [jnp.where(slot == keys[g, pl.ds(2 * a + p, 1), :], 1.0, 0.0).astype(F32) for p in (0, 1)]
            count = hots[0] + hots[1]
            hot = jnp.concatenate(hots, axis=1).astype(BF16)
            total = None
            for level in (0, 1):
                window = [parts[p][level][start : start + LANES] for p in (0, 1)]
                term = dot(hot, jnp.concatenate(window, axis=0))
                total = term if total is None else total + term
            for s in range(3):
                piece, number = total[s * n : (s + 1) * n], count[s * n : (s + 1) * n]
                if s == 2 or a == 0:
                    sums[a + s, low:high, :length] = piece
                    counts[a + s, low:high] = number
                else:
                    sums[a + s, low:high, :length] += piece
                    counts[a + s, low:high] += number
    for r in range(rows // 2 + 2):
        whole = jnp.sum(counts[r], axis=1, keepdims=True)
        sums[r, :, length:] = jnp.broadcast_to(whole, (bins, LANES))
    for load in loads:
        load.wait()


def edges(plane, length, lane0, tail):
    if tail:
        return pltpu.roll(plane[:, length - LANES : length], (lane0 + REACH) % LANES, 1)
    return pltpu.roll(plane[:, :LANES], lane0, 1) if lane0 else plane[:, :LANES]


def edge_kernel(sums, first, last):
    rows, bins, width = sums.shape
    lane = lax.broadcasted_iota(jnp.int32, (bins, LANES), 1)
    for out, tail in ((first, False), (last, True)):
        values = jnp.zeros((bins, LANES), F32)
        for b in range(rows - 2):
            values = jnp.where(lane // REACH == b, edges(sums[b + 1], width - LANES, b * REACH, tail), values)
        out[...] = values


def add_column(values, at_start, sums, first, last):
    rows, bins, width = sums.shape
    length = width - LANES
    sub = lax.broadcasted_iota(jnp.int32, (8, width), 0)
    place = jnp.where(at_start, 0, 7)
    base = pl.multiple_of(jnp.where(at_start, 0, bins - 8), 8)
    there = sub == place
    for b in range(rows - 2):
        gain = jnp.where(there, jnp.broadcast_to(values[b : b + 1], (8, width)), 0.0)
        sums[b + 1, pl.ds(base, 8), :] += gain
    lane = lax.broadcasted_iota(jnp.int32, (8, LANES), 1)
    for edge, tail in ((first, False), (last, True)):
        gain = jnp.zeros((8, LANES), F32)
        for b in range(rows - 2):
            row = edges(values[b : b + 1], length, b * REACH, tail)
            gain = jnp.where(lane // REACH == b, jnp.broadcast_to(row, (8, LANES)), gain)
        edge[pl.ds(base, 8), :] += jnp.where(there[:, :LANES], gain, 0.0)


def join_xl_kernel(sums_in, got, first_in, last_in, sums, payload, first, last):
    rows, bins, _ = sums.shape
    low = lax.axis_index("il") == 0
    above, there = gets()
    count = rows - 2
    values = jnp.where(there, got[...], 0.0)
    payload[:bins, :] = sums[jnp.where(low, rows - 1, 0)]
    payload[bins:, :] = jnp.where(low, values[count:], values[:count])
    add_column(jnp.where(low, values[:count], values[count:]), ~above, sums, first, last)


def join_il_kernel(sums_in, first_in, last_in, got, sums, first, last, one, two):
    rows, bins, width = sums.shape
    length = width - LANES
    low = lax.axis_index("il") == 0
    half = LANES // 2
    add_column(got[bins:], other_at_start(), sums, first, last)
    rim = got[:bins]
    sums[jnp.where(low, rows - 2, 1)] += rim
    lane = lax.broadcasted_iota(jnp.int32, (bins, LANES), 1)
    values = []
    for old, tail in ((first, False), (last, True)):
        edge = edges(rim, length, 0, tail)
        edge = jnp.where(low, pltpu.roll(edge, half - REACH, 1), edge)
        there = lane // REACH == jnp.where(low, half // REACH - 1, 0)
        values.append(packed(old[...] + jnp.where(there, edge, 0.0)))
    one[...] = jnp.where(low, values[1], values[0])
    two[...] = jnp.where(low, values[0], values[1])


def split_row(bins):
    return pl.cdiv(bins, 16) * 8


def packed(values):
    bins = values.shape[0]
    cut = split_row(bins)
    rest = jnp.concatenate([values[cut:], jnp.zeros((2 * cut - bins, LANES), F32)], axis=0)
    lane = lax.broadcasted_iota(jnp.int32, (cut, LANES), 1)
    return jnp.where(lane < LANES // 2, values[:cut], pltpu.roll(rest, LANES // 2, 1))


def unpacked(values, bins):
    return jnp.concatenate([values, pltpu.roll(values, LANES // 2, 1)[: bins - values.shape[0]]], axis=0)


def resample_kernel(sums, table_h, table_l, out, ends, scales, middle, sem):
    rows, bins, width = sums.shape
    length = width - LANES
    count = rows - 2
    out_len = out.shape[2]
    step = 2
    copies = []
    for start in range(0, count, step):
        planes = sums[start + 1 : start + 1 + step]
        scale = 1.0 / jnp.maximum(planes[:, :, length:], 1.0)
        scales[start : start + step] = scale
        values = planes[:, :, :length] * jnp.concatenate([scale] * (length // LANES), axis=2)
        high, low = split(values.reshape(step * bins, length))
        got = dot(high, table_h[...]) + dot(low, table_h[...]) + dot(high, table_l[...])
        got = got.reshape(step, bins, out_len)
        middle[start : start + step] = got[:, :, LANES : out_len - LANES]
        copies.append(
            pltpu.make_async_copy(
                middle.at[start : start + step],
                out.at[start : start + step, :, LANES : out_len - LANES],
                sem.at[start // step],
            )
        )
        copies[-1].start()
        ends[start : start + step, :, :LANES] = got[:, :, :LANES]
        ends[start : start + step, :, LANES:] = got[:, :, out_len - LANES :]
    for copy in copies:
        copy.wait()


def finish_kernel(first_trade, out_in, ends, scales, got, table_h, table_l, out, piece, sem):
    count, bins, _ = ends.shape
    ta = lax.axis_index("ta")
    low = lax.axis_index("il") == 0
    before = low if first_trade else ~low
    there = jnp.where(before, ta > 0, ta < lax.axis_size("ta") - 1)
    values = unpacked(jnp.where(there, got[...], 0.0), bins)
    high, low_part = split(values)
    side = jnp.where(before, 0, 1)
    start_h, start_l = table_h[side], table_l[side]
    fix = dot(high, start_h) + dot(low_part, start_h) + dot(high, start_l)
    fix = jnp.where(before, fix, pltpu.roll(fix, LANES - SPREAD, 1))
    lane = lax.broadcasted_iota(jnp.int32, (bins, LANES), 1)
    here = jnp.where(before, lane, LANES - 1 - lane) < SPREAD
    start = pl.multiple_of(jnp.where(before, 0, out.shape[2] - LANES), LANES)
    copies = []
    for b in range(count):
        base = jnp.where(before, ends[b, :, :LANES], ends[b, :, LANES:])
        moved = pltpu.roll(fix, LANES - b * SPREAD, 1) if b else fix
        piece[b] = base + jnp.where(here, moved, 0.0) * scales[b]
        copies.append(pltpu.make_async_copy(piece.at[b], out.at[b, :, pl.ds(start, LANES)], sem.at[b]))
        copies[-1].start()
    for copy in copies:
        copy.wait()


VMEM = pl.BlockSpec(memory_space=pltpu.VMEM)
HBM = pl.BlockSpec(memory_space=pltpu.HBM)


def call(kernel, ins, outs, scratch=(), aliases={}):
    def run(*args):
        return pl.pallas_call(
            kernel,
            in_specs=ins,
            out_specs=[spec for spec, _ in outs],
            out_shape=[shape for _, shape in outs],
            scratch_shapes=list(scratch),
            input_output_aliases=aliases,
            compiler_params=pltpu.CompilerParams(vmem_limit_bytes=24 << 20),
        )(*args)

    return run


def in_hbm(values):
    return pltpu.with_memory_space_constraint(values, pltpu.HBM)


def vmem(*dims, kind=F32):
    return VMEM, jax.ShapeDtypeStruct(dims, kind)


def shards(sizes, traces, bin_steps):
    return steps_of(sizes, traces, bin_steps)


def steps_of(sizes, traces, bin_steps):
    _, n_xl, n_ta = sizes
    rows, cols, length = traces.shape
    half, bins = rows // 2, cols // 2
    width = length + LANES
    out_len = length * P_SIZE // Q
    main = split_table(main_table(length))
    edge = split_table(edge_table(length, half))
    dma = pltpu.SemaphoreType.DMA

    keep, give = call(
        rim_kernel,
        [HBM, HBM],
        [vmem(rows, width)] * 2,
        [pltpu.VMEM((rows, 8, length), F32)] * 2 + [pltpu.VMEM(bin_steps.shape, jnp.int32), dma((3,))],
    )(in_hbm(traces), in_hbm(bin_steps))
    swap = [(0, 1), (1, 0)]
    chip_rims = keep + lax.ppermute(give, "il", swap)
    came = lax.ppermute(chip_rims, ("il", "xl"), paired(n_xl))

    tables = (*main, *edge)
    sums, *tables = call(
        bin_kernel,
        [VMEM, VMEM] + [HBM] * 4,
        [vmem(half + 2, bins, width)] + [vmem(*t.shape, kind=BF16) for t in tables],
        [pltpu.VMEM((len(groups_of(cols)), rows, LANES), jnp.int32), pltpu.VMEM((half + 2, bins, LANES), F32), dma((4,))],
    )(traces, bin_steps, *[in_hbm(t) for t in tables])
    main, edge = tables[:2], tables[2:]
    first, last = call(edge_kernel, [VMEM], [vmem(bins, LANES)] * 2)(sums)
    sums, payload, first, last = call(
        join_xl_kernel,
        [VMEM] * 4,
        [vmem(half + 2, bins, width), vmem(bins + half, width)] + [vmem(bins, LANES)] * 2,
        aliases={0: 0, 2: 2, 3: 3},
    )(sums, came, first, last)
    got = lax.ppermute(payload, "il", swap)
    sums, first, last, one, two = call(
        join_il_kernel,
        [VMEM] * 4,
        [vmem(half + 2, bins, width)] + [vmem(bins, LANES)] * 2 + [vmem(split_row(bins), LANES)] * 2,
        aliases={0: 0, 1: 1, 2: 2},
    )(sums, first, last, got)
    one = lax.ppermute(one, ("il", "ta"), turning(n_ta))
    two = lax.ppermute(two, ("il", "ta"), [(j, i) for i, j in turning(n_ta)])

    whole = (HBM, jax.ShapeDtypeStruct((half, bins, out_len), F32))
    out, ends, scales = call(
        resample_kernel,
        [VMEM] * 3,
        [whole, vmem(half, bins, 2 * LANES), vmem(half, bins, LANES)],
        [pltpu.VMEM((half, bins, out_len - 2 * LANES), F32), dma((half // 2,))],
    )(sums, *main)
    for first_trade, halo in ((True, one), (False, two)):
        (out,) = call(
            functools.partial(finish_kernel, first_trade),
            [HBM] + [VMEM] * 5,
            [whole],
            [pltpu.VMEM((half, bins, LANES), F32), dma((half,))],
            {0: 0},
        )(out, ends, scales, halo, *edge)
    return out


def turning(count):
    pairs = [(count - 1, 2 * count - 1), (count, 0)]
    for i in range(count - 1):
        pairs += [(i, i + 1), (count + i + 1, count + i)]
    return pairs


def solution(mesh):
    sizes = tuple(mesh.shape[axis] for axis in ("il", "xl", "ta"))
    assert sizes[0] == 2
    return jax.shard_map(
        functools.partial(shards, sizes),
        mesh=mesh,
        in_specs=(P("il", "xl", "ta"), P(None, "il", "xl")),
        out_specs=P("il", "xl", "ta"),
        check_vma=False,
    )
```

```python
import functools

import jax
import jax.numpy as jnp
import numpy as np
from jax import lax
from jax.experimental import pallas as pl
from jax.experimental.pallas import tpu as pltpu
from jax.sharding import PartitionSpec as P


TAPS = 16
P_SIZE = 3
Q = 2
REACH = TAPS // 2
LANES = 128
F32 = jnp.float32
BF16 = jnp.bfloat16
SPREAD = 16


def weight(x):
    inside = np.abs(x) < REACH
    return np.where(inside, np.sinc(x) * np.sinc(x / REACH), 0.0)


def split_table(table):
    high = table.astype(BF16)
    return high, (table - high.astype(np.float64)).astype(BF16)


def main_table(length):
    n = np.arange(length)[:, None]
    m = np.arange(length * P_SIZE // Q)[None, :]
    return weight((m * Q - n * P_SIZE) / P_SIZE)


def edge_table(length, count):
    out_len = length * P_SIZE // Q
    assert count * REACH <= LANES // 2 and count * SPREAD <= LANES and REACH * P_SIZE <= SPREAD * Q
    table = np.zeros((2, LANES, LANES))
    k = np.arange(REACH)[:, None]
    m = np.arange(SPREAD)[None, :]
    before = weight((m * Q - (k - REACH) * P_SIZE) / P_SIZE)
    after = weight(((m + out_len - SPREAD) * Q - (length + k) * P_SIZE) / P_SIZE)
    for b in range(count):
        r, c = b * REACH, b * SPREAD
        table[0, r : r + REACH, c : c + SPREAD] = before
        table[1, r : r + REACH, c : c + SPREAD] = after
    return table


def split(values):
    high = values.astype(BF16)
    return high, (values - high.astype(F32)).astype(BF16)


def dot(a, b, precision=None):
    return jnp.dot(a, b, precision=precision, preferred_element_type=F32)


def sends_up():
    return (lax.axis_index("il") + lax.axis_index("xl")) % 2 == 0


def gets():
    xl, last = lax.axis_index("xl"), lax.axis_size("xl") - 1
    low = lax.axis_index("il") == 0
    end = (xl == 0) | (xl == last)
    return jnp.where(end, xl == 0, sends_up()), ~(end & low)


def other_at_start():
    xl, last = lax.axis_index("xl"), lax.axis_size("xl") - 1
    end = (xl == 0) | (xl == last)
    return jnp.where(end, xl == last, sends_up())


def paired(count):
    assert count % 2 == 0 and count > 2
    last = count - 1
    target = {i: i ^ 1 for i in range(count)}
    for i in range(1, last, 2):
        target[count + i], target[count + i + 1] = count + i + 1, count + i
    for end in (0, last):
        target[end ^ 1] = count + end
        target[count + end] = end
    return sorted(target.items())


def rim_kernel(traces, steps_hbm, keep, give, left, right, steps, sems):
    rows, cols, length = traces.shape
    copies = (
        pltpu.make_async_copy(steps_hbm, steps, sems.at[2]),
        pltpu.make_async_copy(traces.at[:, 0:8, :], left, sems.at[0]),
        pltpu.make_async_copy(traces.at[:, cols - 8 : cols, :], right, sems.at[1]),
    )
    for copy in copies:
        copy.start(priority=1)
    low = lax.axis_index("il") == 0
    up = sends_up()
    g = lax.broadcasted_iota(jnp.int32, (rows, 6 * rows), 0) + jnp.where(low, 1, 1 - rows // 2)
    k = lax.broadcasted_iota(jnp.int32, (rows, 6 * rows), 1) % (3 * rows)
    pick = ((k % rows) // 2 + k // rows == g).astype(F32).astype(BF16)
    copies[0].wait()
    step_il = steps[0]
    step_xl = steps[1]
    masks = {}
    for side, spots in ((-1, (0, 1)), (1, (cols - 2, cols - 1))):
        for j in spots:
            for shift in (-1, 0, 1):
                hit = (step_xl[:, j : j + 1] == side) & (step_il[:, j : j + 1] == shift)
                masks[side, j, shift] = hit.astype(F32)
    copies[1].wait()
    copies[2].wait()
    sides = []
    for side, buf, spots in ((-1, left, ((0, 0), (1, 1))), (1, right, ((cols - 2, 6), (cols - 1, 7)))):
        parts = []
        for shift in (-1, 0, 1):
            total, count = None, None
            for j, place in spots:
                mask = masks[side, j, shift]
                term = buf[:, place, :] * mask
                total = term if total is None else total + term
                count = mask if count is None else count + mask
            parts.append(jnp.concatenate([total, jnp.broadcast_to(count, (rows, LANES))], axis=1))
        sides.append(jnp.concatenate(parts, axis=0))
    both = dot(pick, jnp.concatenate(split(jnp.concatenate(sides, axis=1)), axis=0))
    to_left, to_right = both[:, : length + LANES], both[:, length + LANES :]
    keep[...] = jnp.where(up, to_right, to_left)
    give[...] = jnp.where(up, to_left, to_right)


def groups_of(cols):
    assert cols % 16 == 0 and cols >= LANES
    bins, most, out = cols // 2, LANES // 2 - 8, []
    for low in range(0, bins, most):
        high = min(bins, low + most)
        start = min(max((2 * low - 2) // 16 * 16, 0), cols - LANES)
        assert start <= max(2 * low - 2, 0) and min(2 * high + 2, cols) <= start + LANES
        out.append((low, high, start))
    return out


def add_rows(traces, steps, pairs, fresh, sums, counts, keys):
    rows, cols, length = traces.shape
    groups = groups_of(cols)
    column = lax.broadcasted_iota(jnp.int32, (rows, cols), 1) // 2 + steps[1]
    row = steps[0] + 1
    for g, (low, high, start) in enumerate(groups):
        here, there = column[:, start : start + LANES], row[:, start : start + LANES]
        inside = (here >= low) & (here < high)
        keys[g] = jnp.where(inside, there * (high - low) + here - low, -1)
    fresh = set(fresh)
    for a in pairs:
        parts = [split(traces[2 * a + p]) for p in (0, 1)]
        for g, (low, high, start) in enumerate(groups):
            n = high - low
            slot = lax.broadcasted_iota(jnp.int32, (pl.cdiv(3 * n, 16) * 16, LANES), 0)
            hots = [jnp.where(slot == keys[g, pl.ds(2 * a + p, 1), :], 1.0, 0.0).astype(F32) for p in (0, 1)]
            count = hots[0] + hots[1]
            hot = jnp.concatenate(hots, axis=1).astype(BF16)
            total = None
            for level in (0, 1):
                window = [parts[p][level][start : start + LANES] for p in (0, 1)]
                term = dot(hot, jnp.concatenate(window, axis=0))
                total = term if total is None else total + term
            for s in range(3):
                piece, number = total[s * n : (s + 1) * n], count[s * n : (s + 1) * n]
                if a + s in fresh:
                    sums[a + s, low:high, :length] = piece
                    counts[a + s, low:high] = number
                else:
                    sums[a + s, low:high, :length] += piece
                    counts[a + s, low:high] += number
        fresh -= {a, a + 1, a + 2}


def fold_lanes(counts):
    whole = jnp.sum(counts, axis=1, keepdims=True)
    return jnp.broadcast_to(whole, counts.shape)


def outer_pairs(count):
    return sorted({0, min(1, count - 1), max(count - 2, 0), count - 1})


def bin_outer_kernel(traces, steps, sums, counts, row, keys):
    half = traces.shape[0] // 2
    length = traces.shape[2]
    add_rows(traces, steps, outer_pairs(half), range(half + 2), sums, counts, keys)
    place = jnp.where(lax.axis_index("il") == 0, half + 1, 0)
    row[:, :length] = sums[place, :, :length]
    row[:, length:] = fold_lanes(counts[place])


def bin_inner_kernel(traces, steps, sums_in, counts, sums, keys, number):
    half = traces.shape[0] // 2
    length = traces.shape[2]
    done = outer_pairs(half)
    written = {a + s for a in done for s in range(3)}
    fresh = [r for r in range(half + 2) if r not in written]
    for r in written:
        number[r] = counts[r]
    add_rows(traces, steps, [a for a in range(half) if a not in done], fresh, sums, number, keys)
    for r in range(1, half + 1):
        sums[r, :, length:] = fold_lanes(number[r])


def edges(plane, length, lane0, tail):
    if tail:
        return pltpu.roll(plane[:, length - LANES : length], (lane0 + REACH) % LANES, 1)
    return pltpu.roll(plane[:, :LANES], lane0, 1) if lane0 else plane[:, :LANES]


def edge_kernel(sums_in, rim, sums, first, last):
    rows, bins, width = sums.shape
    sums[jnp.where(lax.axis_index("il") == 0, rows - 2, 1)] += rim[...]
    lane = lax.broadcasted_iota(jnp.int32, (bins, LANES), 1)
    for out, tail in ((first, False), (last, True)):
        values = jnp.zeros((bins, LANES), F32)
        for b in range(rows - 2):
            values = jnp.where(lane // REACH == b, edges(sums[b + 1], width - LANES, b * REACH, tail), values)
        out[...] = packed(values)


def corner(at_start, bins):
    end = bins - 1 - split_row(bins)
    row, lane = jnp.where(at_start, 0, end), jnp.where(at_start, 0, LANES // 2)
    return pl.multiple_of(row // 8 * 8, 8), row % 8, lane


def corner_edges(values, length, row, lane0):
    count = values.shape[0]
    sub = lax.broadcasted_iota(jnp.int32, (8, LANES), 0)
    lane = lax.broadcasted_iota(jnp.int32, (1, LANES), 1)
    out = []
    for tail in (False, True):
        line = jnp.zeros((1, LANES), F32)
        for b in range(count):
            line = jnp.where(lane // REACH == b, edges(values[b : b + 1], length, b * REACH, tail), line)
        line = jnp.where(lane0 == 0, line, pltpu.roll(line, LANES // 2, 1))
        out.append(jnp.where(sub == row, jnp.broadcast_to(line, (8, LANES)), 0.0))
    return out


def join_xl_kernel(got, first_in, last_in, mine, payload, first, last, *, bins):
    width = got.shape[1]
    length = width - LANES
    count = got.shape[0] // 2
    low = lax.axis_index("il") == 0
    above, there = gets()
    values = jnp.where(there, got[...], 0.0)
    other = jnp.where(low, values[count:], values[:count])
    own = jnp.where(low, values[:count], values[count:])
    mine[...] = own
    payload[:, :width] = other
    tile, row, lane0 = corner(~above, bins)
    payload[:, width : width + LANES], payload[:, width + LANES :] = corner_edges(other, length, row, lane0)
    gains = corner_edges(own, length, row, lane0)
    first[pl.ds(tile, 8), :] += gains[0]
    last[pl.ds(tile, 8), :] += gains[1]


def join_il_kernel(first, last, got, one, two, *, bins):
    width = got.shape[1] - 2 * LANES
    even = lax.axis_index("ta") % 2 == 0
    head, tail = first[...], last[...]
    one[...] = jnp.where(even, tail, head)
    two[...] = jnp.where(even, head, tail)
    tile, _, _ = corner(other_at_start(), bins)
    head, tail = got[:, width : width + LANES], got[:, width + LANES :]
    one[pl.ds(tile, 8), :] += jnp.where(even, tail, head)
    two[pl.ds(tile, 8), :] += jnp.where(even, head, tail)


def add_column(values, at_start, sums):
    rows, bins, width = sums.shape
    sub = lax.broadcasted_iota(jnp.int32, (8, width), 0)
    base = pl.multiple_of(jnp.where(at_start, 0, bins - 8), 8)
    there = sub == jnp.where(at_start, 0, 7)
    for b in range(rows - 2):
        gain = jnp.where(there, jnp.broadcast_to(values[b : b + 1], (8, width)), 0.0)
        sums[b + 1, pl.ds(base, 8), :] += gain


def split_row(bins):
    return pl.cdiv(bins, 16) * 8


def packed(values):
    bins = values.shape[0]
    cut = split_row(bins)
    rest = jnp.concatenate([values[cut:], jnp.zeros((2 * cut - bins, LANES), F32)], axis=0)
    lane = lax.broadcasted_iota(jnp.int32, (cut, LANES), 1)
    return jnp.where(lane < LANES // 2, values[:cut], pltpu.roll(rest, LANES // 2, 1))


def unpacked(values, bins):
    return jnp.concatenate([values, pltpu.roll(values, LANES // 2, 1)[: bins - values.shape[0]]], axis=0)


def resample_kernel(sums_in, mine, got, table_h, table_l, sums, tiles, scales):
    rows, bins, width = sums.shape
    add_column(mine[...], ~gets()[0], sums)
    add_column(got[:, :width], other_at_start(), sums)
    length = width - LANES
    count = rows - 2
    step = 2
    for start in range(0, count, step):
        planes = sums[start + 1 : start + 1 + step]
        scale = 1.0 / jnp.maximum(planes[:, :, length:], 1.0)
        scales[start : start + step] = scale
        values = planes[:, :, :length] * jnp.concatenate([scale] * (length // LANES), axis=2)
        high, low = split(values.reshape(step * bins, length))
        got_out = dot(high, table_h[...]) + dot(low, table_h[...]) + dot(high, table_l[...])
        for tile in range(tiles.shape[0]):
            piece = got_out[:, tile * LANES : (tile + 1) * LANES]
            tiles[tile, start : start + step] = piece.reshape(step, bins, LANES)


def end_pieces(first_trade, tiles, scales, got, table_h, table_l):
    count, bins, _ = scales.shape
    ta = lax.axis_index("ta")
    before = ta % 2 == (1 if first_trade else 0)
    there = jnp.where(before, ta > 0, ta < lax.axis_size("ta") - 1)
    values = unpacked(jnp.where(there, got[...], 0.0), bins)
    high, low_part = split(values)
    side = jnp.where(before, 0, 1)
    start_h, start_l = table_h[side], table_l[side]
    fix = dot(high, start_h) + dot(low_part, start_h) + dot(high, start_l)
    fix = jnp.where(before, fix, pltpu.roll(fix, LANES - SPREAD, 1))
    lane = lax.broadcasted_iota(jnp.int32, (bins, LANES), 1)
    here = jnp.where(before, lane, LANES - 1 - lane) < SPREAD
    tile = jnp.where(before, 0, tiles.shape[0] - 1)
    for b in range(count):
        moved = pltpu.roll(fix, LANES - b * SPREAD, 1) if b else fix
        yield tile, b, tiles[tile, b] + jnp.where(here, moved, 0.0) * scales[b]


def to_output(tiles, out, tile, rows, sem):
    start = tile * LANES if isinstance(tile, int) else pl.multiple_of(tile * LANES, LANES)
    return pltpu.make_async_copy(tiles.at[tile, rows], out.at[rows, :, pl.ds(start, LANES)], sem)


def finish_one_kernel(tiles_in, scales, got, table_h, table_l, tiles):
    for tile, b, piece in end_pieces(True, tiles, scales, got, table_h, table_l):
        tiles[tile, b] = piece


def finish_two_kernel(tiles_in, scales, got, table_h, table_l, out, tiles, sems):
    count = scales.shape[0]
    every = pl.ds(0, count)
    ta = lax.axis_index("ta")
    before = ta % 2 == 0
    last = tiles_in.shape[0] - 1
    copies = [to_output(tiles_in, out, n, every, sems.at[count + n]) for n in range(1, last)]
    copies.append(to_output(tiles_in, out, jnp.where(before, last, 0), every, sems.at[count]))
    for copy in copies:
        copy.start()
    for tile, b, piece in end_pieces(False, tiles_in, scales, got, table_h, table_l):
        tiles[b] = piece
        start = pl.multiple_of(tile * LANES, LANES)
        copies.append(pltpu.make_async_copy(tiles.at[b], out.at[b, :, pl.ds(start, LANES)], sems.at[b]))
        copies[-1].start()
    for copy in copies:
        copy.wait()


VMEM = pl.BlockSpec(memory_space=pltpu.VMEM)
HBM = pl.BlockSpec(memory_space=pltpu.HBM)


def call(kernel, ins, outs, scratch=(), aliases={}):
    def run(*args):
        return pl.pallas_call(
            kernel,
            in_specs=ins,
            out_specs=[spec for spec, _ in outs],
            out_shape=[shape for _, shape in outs],
            scratch_shapes=list(scratch),
            input_output_aliases=aliases,
            compiler_params=pltpu.CompilerParams(vmem_limit_bytes=24 << 20),
        )(*args)

    return run


def in_hbm(values):
    return pltpu.with_memory_space_constraint(values, pltpu.HBM)


def vmem(*dims, kind=F32):
    return VMEM, jax.ShapeDtypeStruct(dims, kind)


def shards(sizes, traces, bin_steps):
    return steps_of(sizes, traces, bin_steps)


def steps_of(sizes, traces, bin_steps):
    _, n_xl, n_ta = sizes
    rows, cols, length = traces.shape
    half, bins = rows // 2, cols // 2
    width = length + LANES
    out_len = length * P_SIZE // Q
    main = split_table(main_table(length))
    edge = split_table(edge_table(length, half))
    dma = pltpu.SemaphoreType.DMA

    keep, give = call(
        rim_kernel,
        [HBM, HBM],
        [vmem(rows, width)] * 2,
        [pltpu.VMEM((rows, 8, length), F32)] * 2 + [pltpu.VMEM(bin_steps.shape, jnp.int32), dma((3,))],
    )(in_hbm(traces), in_hbm(bin_steps))
    swap = [(0, 1), (1, 0)]
    shape = (half + 2, bins, width)
    keys = pltpu.VMEM((len(groups_of(cols)), rows, LANES), jnp.int32)
    other = lax.ppermute(give, "il", swap)
    sums, counts, row = call(
        bin_outer_kernel, [VMEM] * 2, [vmem(*shape), vmem(half + 2, bins, LANES), vmem(bins, width)], [keys]
    )(traces, bin_steps)
    came = lax.ppermute(keep + other, ("il", "xl"), paired(n_xl))
    rim = lax.ppermute(row, "il", swap)

    (sums,) = call(
        bin_inner_kernel, [VMEM] * 4, [vmem(*shape)], [keys, pltpu.VMEM((half + 2, bins, LANES), F32)], {2: 0}
    )(traces, bin_steps, sums, counts)
    tall = split_row(bins)
    sums, first, last = call(
        edge_kernel, [VMEM] * 2, [vmem(*shape)] + [vmem(tall, LANES)] * 2, aliases={0: 0}
    )(sums, rim)
    mine, payload, first, last = call(
        functools.partial(join_xl_kernel, bins=bins),
        [VMEM] * 3,
        [vmem(half, width), vmem(half, width + 2 * LANES)] + [vmem(tall, LANES)] * 2,
        aliases={1: 2, 2: 3},
    )(came, first, last)
    got = lax.ppermute(payload, "il", swap)
    one, two = call(functools.partial(join_il_kernel, bins=bins), [VMEM] * 3, [vmem(tall, LANES)] * 2)(first, last, got)
    ones, twos = trades(n_ta)
    one = lax.ppermute(one, ("il", "ta"), ones)
    two = lax.ppermute(two, ("il", "ta"), twos)

    count = out_len // LANES
    sums, tiles, scales = call(
        resample_kernel,
        [VMEM] * 5,
        [vmem(*shape), vmem(count, half, bins, LANES), vmem(half, bins, LANES)],
        aliases={0: 0},
    )(sums, mine, got, *main)
    (tiles,) = call(
        finish_one_kernel, [VMEM] * 5, [vmem(count, half, bins, LANES)], aliases={0: 0}
    )(tiles, scales, one, *edge)
    (out,) = call(
        finish_two_kernel,
        [VMEM] * 5,
        [(HBM, jax.ShapeDtypeStruct((half, bins, out_len), F32))],
        [pltpu.VMEM((half, bins, LANES), F32), dma((half + count,))],
    )(tiles, scales, two, *edge)
    return out


def trades(count):
    assert count % 2 == 0
    one = [(core * count + i, core * count + (i ^ 1)) for core in range(2) for i in range(count)]
    two = [(0, count), (count, 0), (count - 1, 2 * count - 1), (2 * count - 1, count - 1)]
    for core in range(2):
        for i in range(1, count - 1, 2):
            two += [(core * count + i, core * count + i + 1), (core * count + i + 1, core * count + i)]
    return one, two


def solution(mesh):
    sizes = tuple(mesh.shape[axis] for axis in ("il", "xl", "ta"))
    assert sizes[0] == 2
    return jax.shard_map(
        functools.partial(shards, sizes),
        mesh=mesh,
        in_specs=(P("il", "xl", "ta"), P(None, "il", "xl")),
        out_specs=P("il", "xl", "ta"),
        check_vma=False,
    )
```

```python
import functools

import jax
import jax.numpy as jnp
import numpy as np
from jax import lax
from jax.experimental import pallas as pl
from jax.experimental.pallas import tpu as pltpu
from jax.sharding import PartitionSpec as P


TAPS = 16
P_SIZE = 3
Q = 2
REACH = TAPS // 2
LANES = 128
F32 = jnp.float32
BF16 = jnp.bfloat16
SPREAD = 16


def weight(x):
    inside = np.abs(x) < REACH
    return np.where(inside, np.sinc(x) * np.sinc(x / REACH), 0.0)


def split_table(table):
    high = table.astype(BF16)
    return high, (table - high.astype(np.float64)).astype(BF16)


def main_table(length):
    n = np.arange(length)[:, None]
    m = np.arange(length * P_SIZE // Q)[None, :]
    return weight((m * Q - n * P_SIZE) / P_SIZE)


def edge_table(length, count):
    out_len = length * P_SIZE // Q
    assert count * REACH <= LANES // 2 and count * SPREAD <= LANES and REACH * P_SIZE <= SPREAD * Q
    table = np.zeros((2, LANES, 2 * LANES))
    k = np.arange(REACH)[:, None]
    m = np.arange(SPREAD)[None, :]
    before = weight((m * Q - (k - REACH) * P_SIZE) / P_SIZE)
    after = weight(((m + out_len - SPREAD) * Q - (length + k) * P_SIZE) / P_SIZE)
    for part in range(2):
        for b in range(count):
            r = part * LANES // 2 + b * REACH
            c = b * SPREAD
            for side, values in ((0, before), (1, after)):
                to = part * LANES + (c + m[0] - side * SPREAD) % LANES
                table[side, r : r + REACH, to] = values.T
    return table


def split(values):
    high = values.astype(BF16)
    return high, (values - high.astype(F32)).astype(BF16)


def dot(a, b, precision=None):
    return jnp.dot(a, b, precision=precision, preferred_element_type=F32)


def sends_up():
    return (lax.axis_index("il") + lax.axis_index("xl")) % 2 == 0


def gets():
    xl, last = lax.axis_index("xl"), lax.axis_size("xl") - 1
    low = lax.axis_index("il") == 0
    end = (xl == 0) | (xl == last)
    return jnp.where(end, xl == 0, sends_up()), ~(end & low)


def other_at_start():
    xl, last = lax.axis_index("xl"), lax.axis_size("xl") - 1
    end = (xl == 0) | (xl == last)
    return jnp.where(end, xl == last, sends_up())


def paired(count):
    assert count % 2 == 0 and count > 2
    last = count - 1
    target = {i: i ^ 1 for i in range(count)}
    for i in range(1, last, 2):
        target[count + i], target[count + i + 1] = count + i + 1, count + i
    for end in (0, last):
        target[end ^ 1] = count + end
        target[count + end] = end
    return sorted(target.items())


def rim_kernel(traces, steps_hbm, keep, give, left, right, steps, sems):
    rows, cols, length = traces.shape
    step = rows // 4
    copies = [pltpu.make_async_copy(steps_hbm, steps, sems.at[0])]
    for n, start in enumerate(range(0, rows, step)):
        part = pl.ds(start, step)
        copies += [
            pltpu.make_async_copy(traces.at[part, 0:8, :], left.at[part], sems.at[2 * n + 1]),
            pltpu.make_async_copy(traces.at[part, cols - 8 : cols, :], right.at[part], sems.at[2 * n + 2]),
        ]
    for copy in copies:
        copy.start(priority=1)
    low = lax.axis_index("il") == 0
    up = sends_up()
    g = lax.broadcasted_iota(jnp.int32, (rows, 6 * rows), 0) + jnp.where(low, 1, 1 - rows // 2)
    k = lax.broadcasted_iota(jnp.int32, (rows, 6 * rows), 1) % (3 * rows)
    pick = ((k % rows) // 2 + k // rows == g).astype(F32).astype(BF16)
    copies[0].wait()
    step_il = steps[0]
    step_xl = steps[1]
    masks = {}
    for side, spots in ((-1, (0, 1)), (1, (cols - 2, cols - 1))):
        for j in spots:
            for shift in (-1, 0, 1):
                hit = (step_xl[:, j : j + 1] == side) & (step_il[:, j : j + 1] == shift)
                masks[side, j, shift] = hit.astype(F32)
    for copy in copies[1:]:
        copy.wait()
    sides = []
    for side, buf, spots in ((-1, left, ((0, 0), (1, 1))), (1, right, ((cols - 2, 6), (cols - 1, 7)))):
        parts = []
        for shift in (-1, 0, 1):
            total, count = None, None
            for j, place in spots:
                mask = masks[side, j, shift]
                term = buf[:, place, :] * mask
                total = term if total is None else total + term
                count = mask if count is None else count + mask
            parts.append(jnp.concatenate([total, jnp.broadcast_to(count, (rows, LANES))], axis=1))
        sides.append(jnp.concatenate(parts, axis=0))
    both = dot(pick, jnp.concatenate(split(jnp.concatenate(sides, axis=1)), axis=0))
    to_left, to_right = both[:, : length + LANES], both[:, length + LANES :]
    keep[...] = jnp.where(up, to_right, to_left)
    give[...] = jnp.where(up, to_left, to_right)


def groups_of(cols):
    assert cols % 16 == 0 and cols >= LANES
    bins, most, out = cols // 2, LANES // 2 - 8, []
    for low in range(0, bins, most):
        high = min(bins, low + most)
        start = min(max((2 * low - 2) // 16 * 16, 0), cols - LANES)
        assert start <= max(2 * low - 2, 0) and min(2 * high + 2, cols) <= start + LANES
        out.append((low, high, start))
    return out


def add_rows(traces, steps, pairs, fresh, sums, counts, keys):
    rows, cols, length = traces.shape
    groups = groups_of(cols)
    column = lax.broadcasted_iota(jnp.int32, (rows, cols), 1) // 2 + steps[1]
    row = steps[0] + 1
    for g, (low, high, start) in enumerate(groups):
        here, there = column[:, start : start + LANES], row[:, start : start + LANES]
        inside = (here >= low) & (here < high)
        keys[g] = jnp.where(inside, there * (high - low) + here - low, -1)
    fresh = set(fresh)
    for a in pairs:
        parts = [split(traces[2 * a + p]) for p in (0, 1)]
        for g, (low, high, start) in enumerate(groups):
            n = high - low
            slot = lax.broadcasted_iota(jnp.int32, (pl.cdiv(3 * n, 16) * 16, LANES), 0)
            hots = [jnp.where(slot == keys[g, pl.ds(2 * a + p, 1), :], 1.0, 0.0).astype(F32) for p in (0, 1)]
            count = hots[0] + hots[1]
            hot = jnp.concatenate(hots, axis=1).astype(BF16)
            total = None
            for level in (0, 1):
                window = [parts[p][level][start : start + LANES] for p in (0, 1)]
                term = dot(hot, jnp.concatenate(window, axis=0))
                total = term if total is None else total + term
            for s in range(3):
                piece, number = total[s * n : (s + 1) * n], count[s * n : (s + 1) * n]
                if a + s in fresh:
                    sums[a + s, low:high, :length] = piece
                    counts[a + s, low:high] = number
                else:
                    sums[a + s, low:high, :length] += piece
                    counts[a + s, low:high] += number
        fresh -= {a, a + 1, a + 2}


def fold_lanes(counts):
    whole = jnp.sum(counts, axis=1, keepdims=True)
    return jnp.broadcast_to(whole, counts.shape)


def outer_pairs(count):
    return sorted({0, min(1, count - 1), max(count - 2, 0), count - 1})


def bin_outer_kernel(traces, steps, sums, counts, row, keys):
    half = traces.shape[0] // 2
    length = traces.shape[2]
    add_rows(traces, steps, outer_pairs(half), range(half + 2), sums, counts, keys)
    place = jnp.where(lax.axis_index("il") == 0, half + 1, 0)
    row[:, :length] = sums[place, :, :length]
    row[:, length:] = fold_lanes(counts[place])


def bin_inner_kernel(traces, steps, sums_in, counts, sums, keys, number):
    half = traces.shape[0] // 2
    length = traces.shape[2]
    done = outer_pairs(half)
    written = {a + s for a in done for s in range(3)}
    fresh = [r for r in range(half + 2) if r not in written]
    for r in written:
        number[r] = counts[r]
    add_rows(traces, steps, [a for a in range(half) if a not in done], fresh, sums, number, keys)
    for r in range(1, half + 1):
        sums[r, :, length:] = fold_lanes(number[r])


def edges(plane, length, lane0, tail):
    if tail:
        return pltpu.roll(plane[:, length - LANES : length], (lane0 + REACH) % LANES, 1)
    return pltpu.roll(plane[:, :LANES], lane0, 1) if lane0 else plane[:, :LANES]


def edge_kernel(sums_in, rim, sums, first, last):
    rows, bins, width = sums.shape
    sums[jnp.where(lax.axis_index("il") == 0, rows - 2, 1)] += rim[...]
    lane = lax.broadcasted_iota(jnp.int32, (bins, LANES), 1)
    for out, tail in ((first, False), (last, True)):
        values = jnp.zeros((bins, LANES), F32)
        for b in range(rows - 2):
            values = jnp.where(lane // REACH == b, edges(sums[b + 1], width - LANES, b * REACH, tail), values)
        out[...] = packed(values)


def corner(at_start, bins):
    end = bins - 1 - split_row(bins)
    row, lane = jnp.where(at_start, 0, end), jnp.where(at_start, 0, LANES // 2)
    return pl.multiple_of(row // 8 * 8, 8), row % 8, lane


def corner_edges(values, length, row, lane0):
    count = values.shape[0]
    sub = lax.broadcasted_iota(jnp.int32, (8, LANES), 0)
    lane = lax.broadcasted_iota(jnp.int32, (1, LANES), 1)
    out = []
    for tail in (False, True):
        line = jnp.zeros((1, LANES), F32)
        for b in range(count):
            line = jnp.where(lane // REACH == b, edges(values[b : b + 1], length, b * REACH, tail), line)
        line = jnp.where(lane0 == 0, line, pltpu.roll(line, LANES // 2, 1))
        out.append(jnp.where(sub == row, jnp.broadcast_to(line, (8, LANES)), 0.0))
    return out


def join_xl_kernel(got, first_in, last_in, mine, payload, first, last, *, bins):
    width = got.shape[1]
    length = width - LANES
    count = got.shape[0] // 2
    low = lax.axis_index("il") == 0
    above, there = gets()
    values = jnp.where(there, got[...], 0.0)
    other = jnp.where(low, values[count:], values[:count])
    own = jnp.where(low, values[:count], values[count:])
    mine[...] = own
    payload[:, :width] = other
    tile, row, lane0 = corner(~above, bins)
    payload[:, width : width + LANES], payload[:, width + LANES :] = corner_edges(other, length, row, lane0)
    gains = corner_edges(own, length, row, lane0)
    first[pl.ds(tile, 8), :] += gains[0]
    last[pl.ds(tile, 8), :] += gains[1]


def join_il_kernel(first, last, got, one, two, *, bins):
    width = got.shape[1] - 2 * LANES
    even = lax.axis_index("ta") % 2 == 0
    head, tail = first[...], last[...]
    one[...] = jnp.where(even, tail, head)
    two[...] = jnp.where(even, head, tail)
    tile, _, _ = corner(other_at_start(), bins)
    head, tail = got[:, width : width + LANES], got[:, width + LANES :]
    one[pl.ds(tile, 8), :] += jnp.where(even, tail, head)
    two[pl.ds(tile, 8), :] += jnp.where(even, head, tail)


def add_column(values, at_start, sums):
    rows, bins, width = sums.shape
    sub = lax.broadcasted_iota(jnp.int32, (8, width), 0)
    base = pl.multiple_of(jnp.where(at_start, 0, bins - 8), 8)
    there = sub == jnp.where(at_start, 0, 7)
    for b in range(rows - 2):
        gain = jnp.where(there, jnp.broadcast_to(values[b : b + 1], (8, width)), 0.0)
        sums[b + 1, pl.ds(base, 8), :] += gain


def split_row(bins):
    return pl.cdiv(bins, 16) * 8


def packed(values):
    bins = values.shape[0]
    cut = split_row(bins)
    rest = jnp.concatenate([values[cut:], jnp.zeros((2 * cut - bins, LANES), F32)], axis=0)
    lane = lax.broadcasted_iota(jnp.int32, (cut, LANES), 1)
    return jnp.where(lane < LANES // 2, values[:cut], pltpu.roll(rest, LANES // 2, 1))


def resample_kernel(sums_in, mine, got, table_h, table_l, sums, tiles, scales, out, sems):
    rows, bins, width = sums.shape
    add_column(mine[...], ~gets()[0], sums)
    add_column(got[:, :width], other_at_start(), sums)
    length = width - LANES
    count = rows - 2
    step = 2
    copies = []
    for start in range(0, count, step):
        planes = sums[start + 1 : start + 1 + step]
        scale = 1.0 / jnp.maximum(planes[:, :, length:], 1.0)
        scales[start : start + step] = scale
        values = planes[:, :, :length] * jnp.concatenate([scale] * (length // LANES), axis=2)
        high, low = split(values.reshape(step * bins, length))
        got_out = dot(high, table_h[...]) + dot(low, table_h[...]) + dot(high, table_l[...])
        for tile in range(tiles.shape[0]):
            piece = got_out[:, tile * LANES : (tile + 1) * LANES]
            tiles[tile, start : start + step] = piece.reshape(step, bins, LANES)
        for tile in range(1, tiles.shape[0] - 1):
            for b in range(start, start + step):
                copies.append(to_output(tiles, out, tile, b, sems.at[tile - 1, b]))
                copies[-1].start()
    for copy in copies:
        copy.wait()


def end_pieces(first_trade, tiles, scales, got, table_h, table_l):
    count, bins, _ = scales.shape
    ta = lax.axis_index("ta")
    before = ta % 2 == (1 if first_trade else 0)
    there = jnp.where(before, ta > 0, ta < lax.axis_size("ta") - 1)
    high, low_part = split(jnp.where(there, got[...], 0.0))
    side = jnp.where(before, 0, 1)
    start_h, start_l = table_h[side], table_l[side]
    fix = dot(high, start_h) + dot(low_part, start_h) + dot(high, start_l)
    fix = jnp.concatenate([fix[:, :LANES], fix[: bins - fix.shape[0], LANES:]], axis=0)
    lane = lax.broadcasted_iota(jnp.int32, (bins, LANES), 1)
    here = jnp.where(before, lane, LANES - 1 - lane) < SPREAD
    tile = jnp.where(before, 0, tiles.shape[0] - 1)
    for b in range(count):
        moved = pltpu.roll(fix, LANES - b * SPREAD, 1) if b else fix
        yield tile, b, tiles[tile, b] + jnp.where(here, moved, 0.0) * scales[b]


def to_output(tiles, out, tile, b, sem):
    start = tile * LANES if isinstance(tile, int) else pl.multiple_of(tile * LANES, LANES)
    return pltpu.make_async_copy(tiles.at[tile, b], out.at[b, :, pl.ds(start, LANES)], sem)


def finish_one_kernel(tiles_in, scales, got, table_h, table_l, tiles):
    for tile, b, piece in end_pieces(True, tiles, scales, got, table_h, table_l):
        tiles[tile, b] = piece


def finish_two_kernel(out_in, tiles_in, scales, got, table_h, table_l, out, tiles, sems):
    count = scales.shape[0]
    ta = lax.axis_index("ta")
    before = ta % 2 == 0
    last = tiles_in.shape[0] - 1
    tile = jnp.where(before, last, 0)
    copies = [to_output(tiles_in, out, tile, b, sems.at[1, b]) for b in range(count)]
    for copy in copies:
        copy.start()
    for tile, b, piece in end_pieces(False, tiles_in, scales, got, table_h, table_l):
        tiles[b] = piece
        start = pl.multiple_of(tile * LANES, LANES)
        copies.append(pltpu.make_async_copy(tiles.at[b], out.at[b, :, pl.ds(start, LANES)], sems.at[0, b]))
        copies[-1].start()
    for copy in copies:
        copy.wait()


VMEM = pl.BlockSpec(memory_space=pltpu.VMEM)
HBM = pl.BlockSpec(memory_space=pltpu.HBM)


def call(kernel, ins, outs, scratch=(), aliases={}):
    def run(*args):
        return pl.pallas_call(
            kernel,
            in_specs=ins,
            out_specs=[spec for spec, _ in outs],
            out_shape=[shape for _, shape in outs],
            scratch_shapes=list(scratch),
            input_output_aliases=aliases,
            compiler_params=pltpu.CompilerParams(vmem_limit_bytes=24 << 20),
        )(*args)

    return run


def in_hbm(values):
    return pltpu.with_memory_space_constraint(values, pltpu.HBM)


def vmem(*dims, kind=F32):
    return VMEM, jax.ShapeDtypeStruct(dims, kind)


def shards(sizes, traces, bin_steps):
    return steps_of(sizes, traces, bin_steps)


def steps_of(sizes, traces, bin_steps):
    _, n_xl, n_ta = sizes
    rows, cols, length = traces.shape
    half, bins = rows // 2, cols // 2
    width = length + LANES
    out_len = length * P_SIZE // Q
    main = split_table(main_table(length))
    edge = split_table(edge_table(length, half))
    dma = pltpu.SemaphoreType.DMA

    keep, give = call(
        rim_kernel,
        [HBM, HBM],
        [vmem(rows, width)] * 2,
        [pltpu.VMEM((rows, 8, length), F32)] * 2 + [pltpu.VMEM(bin_steps.shape, jnp.int32), dma((9,))],
    )(in_hbm(traces), in_hbm(bin_steps))
    swap = [(0, 1), (1, 0)]
    shape = (half + 2, bins, width)
    keys = pltpu.VMEM((len(groups_of(cols)), rows, LANES), jnp.int32)
    other = lax.ppermute(give, "il", swap)
    sums, counts, row = call(
        bin_outer_kernel, [VMEM] * 2, [vmem(*shape), vmem(half + 2, bins, LANES), vmem(bins, width)], [keys]
    )(traces, bin_steps)
    came = lax.ppermute(keep + other, ("il", "xl"), paired(n_xl))
    rim = lax.ppermute(row, "il", swap)

    (sums,) = call(
        bin_inner_kernel, [VMEM] * 4, [vmem(*shape)], [keys, pltpu.VMEM((half + 2, bins, LANES), F32)], {2: 0}
    )(traces, bin_steps, sums, counts)
    tall = split_row(bins)
    sums, first, last = call(
        edge_kernel, [VMEM] * 2, [vmem(*shape)] + [vmem(tall, LANES)] * 2, aliases={0: 0}
    )(sums, rim)
    mine, payload, first, last = call(
        functools.partial(join_xl_kernel, bins=bins),
        [VMEM] * 3,
        [vmem(half, width), vmem(half, width + 2 * LANES)] + [vmem(tall, LANES)] * 2,
        aliases={1: 2, 2: 3},
    )(came, first, last)
    got = lax.ppermute(payload, "il", swap)
    one, two = call(functools.partial(join_il_kernel, bins=bins), [VMEM] * 3, [vmem(tall, LANES)] * 2)(first, last, got)
    ones, twos = trades(n_ta)
    one = lax.ppermute(one, ("il", "ta"), ones)
    two = lax.ppermute(two, ("il", "ta"), twos)

    count = out_len // LANES
    whole = (HBM, jax.ShapeDtypeStruct((half, bins, out_len), F32))
    sums, tiles, scales, out = call(
        resample_kernel,
        [VMEM] * 5,
        [vmem(*shape), vmem(count, half, bins, LANES), vmem(half, bins, LANES), whole],
        [dma((count - 2, half))],
        {0: 0},
    )(sums, mine, got, *main)
    (tiles,) = call(
        finish_one_kernel, [VMEM] * 5, [vmem(count, half, bins, LANES)], aliases={0: 0}
    )(tiles, scales, one, *edge)
    (out,) = call(
        finish_two_kernel, [HBM] + [VMEM] * 5, [whole], [pltpu.VMEM((half, bins, LANES), F32), dma((2, half))], {0: 0}
    )(out, tiles, scales, two, *edge)
    return out


def trades(count):
    assert count % 2 == 0
    one = [(core * count + i, core * count + (i ^ 1)) for core in range(2) for i in range(count)]
    two = [(0, count), (count, 0), (count - 1, 2 * count - 1), (2 * count - 1, count - 1)]
    for core in range(2):
        for i in range(1, count - 1, 2):
            two += [(core * count + i, core * count + i + 1), (core * count + i + 1, core * count + i)]
    return one, two


def solution(mesh):
    sizes = tuple(mesh.shape[axis] for axis in ("il", "xl", "ta"))
    assert sizes[0] == 2
    return jax.shard_map(
        functools.partial(shards, sizes),
        mesh=mesh,
        in_specs=(P("il", "xl", "ta"), P(None, "il", "xl")),
        out_specs=P("il", "xl", "ta"),
        check_vma=False,
    )
```
